32 devices in a mesh: dp: 4 (over z), tensor: 8 (over y, x, core).
Axes of the slice: x: 2, y: 2, z: 4, core: 2. Of those that a mesh axis runs over, the one named last changes fastest.
Arguments:
- inputs: bfloat16 [8192, 2048], P(('dp', 'tensor')), may hold values from -6 to 6
- doc_lengths: int32 [8, 8], P('dp'), may hold values from 1 to 512, 1024 in all within a row
- attn_gain: bfloat16 [2048], replicated, may hold values from 0.099609375 to 1.8984375
- attn_shift: bfloat16 [2048], replicated, may hold values from -1.5 to 1.5
- qkv_weight: bfloat16 [2048, 3, 2048], P(None, None, 'tensor'), may hold values from -0.1875 to 0.1875
- qv_bias: bfloat16 [2, 2048], P(None, 'tensor'), may hold values from -2.5 to 2.5
- out_weight: bfloat16 [2048, 2048], P('tensor'), may hold values from -0.5 to 0.5
- out_bias: bfloat16 [2048], replicated, may hold values from -1.5 to 1.5
- mlp_gain: bfloat16 [2048], replicated, may hold values from 0.099609375 to 1.8984375
- mlp_shift: bfloat16 [2048], replicated, may hold values from -1.5 to 1.5
- up_weight: bfloat16 [2048, 8192], P(None, 'tensor'), may hold values from -0.125 to 0.125
- up_bias: bfloat16 [8192], P('tensor'), may hold values from -2.5 to 2.5
- down_weight: bfloat16 [8192, 2048], P('tensor'), may hold values from -0.09375 to 0.09375
- down_bias: bfloat16 [2048], replicated, may hold values from -1.5 to 1.5
- out_grad: bfloat16 [8192, 2048], P(('dp', 'tensor')), may hold values from -6 to 6
Outputs:
- outputs: bfloat16 [8192, 2048], P(('dp', 'tensor'))
- input_grad: float32 [8192, 2048], P(('dp', 'tensor'))
- attn_gain_grad: float32 [2048], replicated
- attn_shift_grad: float32 [2048], replicated
- qkv_weight_grad: float32 [2048, 3, 2048], P(None, None, 'tensor')
- qv_bias_grad: float32 [2, 2048], P(None, 'tensor')
- out_weight_grad: float32 [2048, 2048], P('tensor')
- out_bias_grad: float32 [2048], replicated
- mlp_gain_grad: float32 [2048], replicated
- mlp_shift_grad: float32 [2048], replicated
- up_weight_grad: float32 [2048, 8192], P(None, 'tensor')
- up_bias_grad: float32 [8192], P('tensor')
- down_weight_grad: float32 [8192, 2048], P('tensor')
- down_bias_grad: float32 [2048], replicated
The draws below stay inside these ranges and needn't reach their ends.
Inputs may be any that keep to these rules, and one draw needn't show every extreme that they name: `doc_lengths`: each row's 8 lengths sum to 1024, and the longest document of every row has exactly 512 tokens.
All inputs are finite; a program needn't handle non-finite values.
Results may differ from the reference program's by a relative error of at most 0.012.
The reference program's roundings to bfloat16 on the way count: a program that leaves them out, or rounds other values in their place, can miss the bound.
Values may be sent and summed in bfloat16 or wider, within the bound.
A program may use at most 192 MiB of HBM per device.

```python
import math
import jax
import jax.numpy as jnp
import numpy as np
from jax import lax

D = 2048
HEADS = 16
HD = 128
FF = 8192
SEQ = 1024
DOCS = 8
MOST_DOC = 512
ROWS_DEV = 2
ROWS = 8
TOKENS = 8192


def shard_levels(key, extent, split, low, top_value):
    def one(position, parts):
        steps = jax.random.uniform(jax.random.fold_in(jax.random.fold_in(key, 6), position), (parts,), jnp.float32, low / len(split), top_value / len(split))
        return jnp.repeat(jnp.exp(steps), extent[position] // parts).reshape((-1,) + (1,) * (len(extent) - position - 1))

    loudness = one(*split[0])
    for cut in split[1:]:
        loudness = loudness * one(*cut)
    return loudness


def length_profile(amount, total, reach, lean):
    portions = [(1 << 20) // math.isqrt(grade ** lean) + 1 for grade in range(2, amount + 1)]
    spare, counts = total - reach - (amount - 1), [1] * (amount - 1)
    while spare > 0:
        movable = [i for i in range(amount - 1) if counts[i] < reach]
        whole, remaining = sum([portions[i] for i in movable]), spare
        for i in movable:
            more = min(reach - counts[i], max(1, remaining * portions[i] // whole), spare)
            counts[i] = counts[i] + more
            spare = spare - more
    return np.array([reach] + counts)


def ragged_sizes(own_key, count, total, reach, skew):
    if count == 2:
        one = jax.random.randint(own_key, (), max(1, total - reach), min(reach, total - 1) + 1)
        return jnp.stack([one, total - one])
    sizes = jnp.asarray(length_profile(count, total, reach, skew), jnp.int32)
    pairs = (count - 1) // 2
    giver, receiver = sizes[1:1 + 2 * pairs:2], sizes[2:2 + 2 * pairs:2]
    slack = jnp.minimum(giver - 1, reach - receiver)
    passed = jax.random.randint(jax.random.fold_in(own_key, 1), (pairs,), 0, 1 << 20) % (slack + 1)
    sizes = sizes.at[1:1 + 2 * pairs:2].set(giver - passed).at[2:2 + 2 * pairs:2].set(receiver + passed)
    return sizes[jax.random.permutation(jax.random.fold_in(own_key, 2), count)]


def scatter_about(own_key, dims, spread, limit, shards=(), kind=jnp.bfloat16):
    factor_of = shard_levels(own_key, dims, shards, -0.22, 0.18) if shards else 1.0
    values = jax.random.normal(own_key, dims, jnp.float32) * spread * factor_of
    return jnp.minimum(jnp.maximum(values, -limit), limit).astype(kind)


def setup_inputs(seed: int = 0) -> dict:
    arg_keys = jax.random.split(jax.random.key(seed), 16)
    return {
        "inputs": scatter_about(arg_keys[0], (TOKENS, D), 1.0, 6.0, ((0, 32),)),
        "doc_lengths": jax.vmap(lambda own: ragged_sizes(own, DOCS, SEQ, MOST_DOC, 2))(jax.random.split(arg_keys[1], ROWS)).reshape((ROWS, DOCS)).astype(jnp.int32),
        "attn_gain": jnp.clip(1.0 + 0.18 * jax.random.normal(arg_keys[2], (D,), jnp.float32), 0.099609375, 1.8984375).astype(jnp.bfloat16),
        "attn_shift": scatter_about(arg_keys[3], (D,), 0.3, 1.5),
        "qkv_weight": scatter_about(arg_keys[4], (D, 3, D), (D // 2) ** -0.5, 0.1875, ((2, 8),)),
        "qv_bias": scatter_about(arg_keys[5], (2, D), 0.5, 2.5, ((1, 8),)),
        "out_weight": scatter_about(arg_keys[6], (D, D), (D // 16) ** -0.5, 0.5, ((0, 8),)),
        "out_bias": scatter_about(arg_keys[7], (D,), 0.3, 1.5),
        "mlp_gain": jnp.clip(1.0 + 0.18 * jax.random.normal(arg_keys[8], (D,), jnp.float32), 0.099609375, 1.8984375).astype(jnp.bfloat16),
        "mlp_shift": scatter_about(arg_keys[9], (D,), 0.3, 1.5),
        "up_weight": scatter_about(arg_keys[10], (D, FF), D ** -0.5, 0.125, ((1, 8),)),
        "up_bias": scatter_about(arg_keys[11], (FF,), 0.5, 2.5, ((0, 8),)),
        "down_weight": scatter_about(arg_keys[12], (FF, D), (FF // 2) ** -0.5, 0.09375, ((0, 8),)),
        "down_bias": scatter_about(arg_keys[13], (D,), 0.3, 1.5),
        "out_grad": scatter_about(arg_keys[14], (TOKENS, D), 1.0, 6.0, ((0, 32),)),
    }


@jax.custom_vjp
def low(v):
    return lax.optimization_barrier(v.astype(jnp.bfloat16)).astype(jnp.float32)

@jax.custom_vjp
def low_back(v):
    return v

def low_keep(v):
    return (low(v), None)

def low_pass(kept, grad):
    return (grad,)

def back_keep(v):
    return (v, None)

def back_low(kept, grad):
    return (low(grad),)
low.defvjp(low_keep, low_pass)
low_back.defvjp(back_keep, back_low)
NORM_EPS = 1e-05
PRECISE = lax.Precision.HIGHEST

def layer_norm(values, gain_vec, shift_vec):
    row_mean = lax.optimization_barrier(jnp.mean(values, axis=-1, keepdims=True))
    centred = values - row_mean
    variance = lax.optimization_barrier(jnp.mean(centred * centred, axis=-1, keepdims=True))
    return centred * lax.rsqrt(variance + NORM_EPS) * gain_vec + shift_vec

def allowed_pairs(lengths):
    doc_ends = jnp.cumsum(lengths, dtype=jnp.int32)
    positions = jnp.arange(SEQ, dtype=jnp.int32)
    doc_ids = lax.optimization_barrier(jnp.sum((positions[:, None] >= doc_ends[None, :]).astype(jnp.int32), axis=1))
    return (doc_ids[:, None] == doc_ids[None, :]) & (positions[None, :] <= positions[:, None])

def row_attention(query_rows, key_rows, value_rows, lengths):
    raw_scores = jnp.einsum('qhd,khd->hqk', query_rows, key_rows, precision=PRECISE) * HD ** (-0.5)
    scores = low_back(raw_scores)
    scores = jnp.where(allowed_pairs(lengths)[None], scores, -1000000000.0)
    row_max = lax.optimization_barrier(jnp.max(scores, axis=-1, keepdims=True))
    exp_scores = jnp.exp(scores - row_max)
    softmax_out = exp_scores / lax.optimization_barrier(jnp.sum(exp_scores, axis=-1, keepdims=True))
    return jnp.einsum('hqk,khd->qhd', low(softmax_out), value_rows, precision=PRECISE)

def attend_packed(scan_item):
    return row_attention(scan_item[0], scan_item[1], scan_item[2], scan_item[3])

def block_forward(values_in, lengths, attn_gain, attn_shift, qkv_weight, qv_bias, out_weight, out_bias, mlp_gain, mlp_shift, up_weight, up_bias, down_weight, down_bias):
    token_count = values_in.shape[0]
    attn_normed = low(layer_norm(values_in, attn_gain, attn_shift))
    joined = jnp.dot(attn_normed, qkv_weight.reshape(D, 3 * D), precision=PRECISE).reshape(token_count, 3, D)
    query_rows = low(low_back(joined[:, 0] + qv_bias[0]))
    key_rows = low(low_back(joined[:, 1]))
    value_rows = low(low_back(joined[:, 2] + qv_bias[1]))
    row_shape = (token_count // SEQ, SEQ, HEADS, HD)
    mixed_rows = lax.map(jax.checkpoint(attend_packed), (query_rows.reshape(row_shape), key_rows.reshape(row_shape), value_rows.reshape(row_shape), lengths))
    heads_out = low(low_back(mixed_rows.reshape(token_count, D)))
    middle = values_in + low_back(jnp.dot(heads_out, out_weight, precision=PRECISE)) + out_bias
    mlp_normed = low(layer_norm(middle, mlp_gain, mlp_shift))
    pre_act = low_back(jnp.dot(mlp_normed, up_weight, precision=PRECISE) + up_bias)
    hidden = low(jax.nn.gelu(pre_act, approximate=True))
    return middle + low_back(jnp.dot(hidden, down_weight, precision=PRECISE)) + down_bias

def reference(inputs, doc_lengths, attn_gain, attn_shift, qkv_weight, qv_bias, out_weight, out_bias, mlp_gain, mlp_shift, up_weight, up_bias, down_weight, down_bias, out_grad):
    params = tuple((param.astype(jnp.float32) for param in (attn_gain, attn_shift, qkv_weight, qv_bias, out_weight, out_bias, mlp_gain, mlp_shift, up_weight, up_bias, down_weight, down_bias)))
    group_count = ROWS // ROWS_DEV
    span = ROWS_DEV * SEQ
    stacked_in = inputs.astype(jnp.float32).reshape(group_count, span, D)
    stacked_grad = out_grad.astype(jnp.float32).reshape(group_count, span, D)
    stacked_len = doc_lengths.reshape(group_count, ROWS_DEV, DOCS)

    def one_group(running, scan_item):
        block_in, block_grad, block_len = scan_item

        def forward_fn(values_in, *weights):
            return block_forward(values_in, block_len, *weights)
        result, pullback = jax.vjp(forward_fn, block_in, *params)
        gradients = pullback(block_grad)
        running = tuple((prior + update for prior, update in zip(running, gradients[1:])))
        return (running, (result, gradients[0]))
    initial = tuple((jnp.zeros_like(param) for param in params))
    running, (results, in_grads) = lax.scan(one_group, initial, (stacked_in, stacked_grad, stacked_len))
    return (results.reshape(TOKENS, D).astype(jnp.bfloat16), in_grads.reshape(TOKENS, D), running[0], running[1], running[2], running[3], running[4], running[5], running[6], running[7], running[8], running[9], running[10], running[11])
```

```python
import functools

import jax
import jax.numpy as jnp
from jax import lax
from jax.experimental import pallas as pl
from jax.experimental.pallas import tpu as pltpu
from jax.sharding import PartitionSpec as P

HD = 128
MOST_DOC = 512
QUERY_BLOCK = 256
NORM_EPS = 1e-05
LOW = jnp.bfloat16
MESH = pl.DeviceIdType.MESH


def positions():
    me = lax.axis_index("tensor")
    core = me % 2
    col = (me // 2) % 2
    row = me // 4
    def at(r, x, c):
        return r * 4 + x * 2 + c
    return me, core, col, row, at

def greet(peers):
    barrier = pltpu.get_barrier_semaphore()
    for peer in peers:
        pl.semaphore_signal(barrier, inc=1, device_id={"tensor": peer}, device_id_type=MESH)
    pl.semaphore_wait(barrier, len(peers))

def gather_kernel(rows, x_ref, o_ref, send, recv, local):
    me, c, x, y, at = positions()
    tx, ty, tc = at(y, 1 - x, c), at(1 - y, x, c), at(y, x, 1 - c)
    td = at(1 - y, 1 - x, c)
    txc, tyc, tdc = at(y, 1 - x, 1 - c), at(1 - y, x, 1 - c), at(1 - y, 1 - x, 1 - c)
    half = rows // 2
    greet((tx, ty, tc))

    def place(block, part):
        return o_ref.at[pl.ds(pl.multiple_of(block * rows + part * half, half), half), :]

    def copy(src, block, part, index, peer):
        return pltpu.make_async_remote_copy(
            src_ref=src, dst_ref=place(block, part), send_sem=send.at[index],
            recv_sem=recv.at[index], device_id={"tensor": peer}, device_id_type=MESH)

    def own(part):
        return x_ref.at[pl.ds(part * half, half), :]

    keep = pltpu.make_async_copy(x_ref, o_ref.at[pl.ds(pl.multiple_of(me * rows, rows), rows), :], local)
    sx0 = copy(own(0), me, 0, 0, tx)
    sy1 = copy(own(1), me, 1, 1, ty)
    sx1 = copy(own(1), me, 1, 2, tx)
    sy0 = copy(own(0), me, 0, 3, ty)
    sc0 = copy(own(0), me, 0, 4, tc)
    sc1 = copy(own(1), me, 1, 5, tc)
    for s in (sx0, sy1, sx1, sy0, sc0, sc1):
        s.start()
    keep.start()
    fy = copy(place(tx, 0), tx, 0, 6, ty)
    fx = copy(place(ty, 1), ty, 1, 7, tx)
    cx0 = copy(place(tx, 0), tx, 0, 8, tc)
    cy1 = copy(place(ty, 1), ty, 1, 9, tc)
    cx1 = copy(place(tx, 1), tx, 1, 10, tc)
    cy0 = copy(place(ty, 0), ty, 0, 11, tc)
    cd0 = copy(place(td, 0), td, 0, 12, tc)
    cd1 = copy(place(td, 1), td, 1, 13, tc)
    sx0.wait_recv()
    fy.start()
    cx0.start()
    sy1.wait_recv()
    fx.start()
    cy1.start()
    sx1.wait_recv()
    cx1.start()
    sy0.wait_recv()
    cy0.start()
    fy.wait_recv()
    cd0.start()
    fx.wait_recv()
    cd1.start()
    for s in (sc0, sc1, cx0, cy1, cx1, cy0, cd0, cd1):
        s.wait_recv()
    for s in (sx0, sy1, sx1, sy0, sc0, sc1, fy, fx, cx0, cy1, cx1, cy0, cd0, cd1):
        s.wait_send()
    keep.wait()

def gather_rows(x, ident):
    rows, width = x.shape
    return pl.pallas_call(
        functools.partial(gather_kernel, rows),
        out_shape=jax.ShapeDtypeStruct((8 * rows, width), x.dtype),
        in_specs=[pl.BlockSpec(memory_space=pl.ANY)],
        out_specs=pl.BlockSpec(memory_space=pl.ANY),
        scratch_shapes=[pltpu.SemaphoreType.DMA((14,)), pltpu.SemaphoreType.DMA((14,)), pltpu.SemaphoreType.DMA],
        compiler_params=pltpu.CompilerParams(collective_id=ident, has_side_effects=True),
    )(x)

TILE = 32
def scatter_kernel(rows, p_ref, o_ref, mine, from_core, total, from_x, from_y, send, recv, local):
    me, c, x, y, at = positions()
    tx, ty, tc = at(y, 1 - x, c), at(1 - y, x, c), at(y, x, 1 - c)
    half = rows // 2
    greet((tx, ty, tc))
    chips = ((1 - y, 1 - x), (y, 1 - x), (1 - y, x), (y, x))

    def block(r, xx, cc):
        return p_ref.at[pl.ds(pl.multiple_of(at(r, xx, cc) * rows, rows), rows), :]

    def remote(src, dst, index, peer):
        return pltpu.make_async_remote_copy(
            src_ref=src, dst_ref=dst, send_sem=send.at[index],
            recv_sem=recv.at[index], device_id={"tensor": peer}, device_id_type=MESH)

    swaps = [remote(block(*chips[k], 1 - c), from_core.at[k], k, tc) for k in range(4)]
    loads = [pltpu.make_async_copy(block(*chips[k], c), mine.at[k], local.at[k]) for k in range(4)]
    for k in range(4):
        swaps[k].start()
        loads[k].start()

    def add(dst, start, size, *srcs):
        @pl.loop(0, size // TILE)
        def _(i):
            base = pl.multiple_of(start + i * TILE, TILE)
            acc = srcs[0][pl.ds(base, TILE), :].astype(jnp.float32)
            for s in srcs[1:]:
                acc = acc + s[pl.ds(base, TILE), :].astype(jnp.float32)
            dst[pl.ds(base, TILE), :] = acc.astype(dst.dtype)

    lo, hi = pl.ds(0, half), pl.ds(half, half)
    dx = remote(total.at[0, lo, :], from_x.at[1, lo, :], 4, tx)
    dy = remote(total.at[0, hi, :], from_y.at[1, hi, :], 5, ty)
    xl = remote(total.at[1, lo, :], from_x.at[0, lo, :], 6, tx)
    xh = remote(total.at[1, hi, :], from_x.at[0, hi, :], 7, tx)
    yl = remote(total.at[2, lo, :], from_y.at[0, lo, :], 8, ty)
    yh = remote(total.at[2, hi, :], from_y.at[0, hi, :], 9, ty)

    swaps[0].wait_recv()
    loads[0].wait()
    add(total.at[0], 0, half, mine.at[0], from_core.at[0])
    dx.start()
    add(total.at[0], half, half, mine.at[0], from_core.at[0])
    dy.start()
    swaps[1].wait_recv()
    loads[1].wait()
    add(total.at[1], 0, half, mine.at[1], from_core.at[1])
    xl.start()
    swaps[2].wait_recv()
    loads[2].wait()
    add(total.at[2], half, half, mine.at[2], from_core.at[2])
    yh.start()
    dy.wait_recv()
    add(total.at[1], half, half, mine.at[1], from_core.at[1], from_y.at[1])
    xh.start()
    dx.wait_recv()
    add(total.at[2], 0, half, mine.at[2], from_core.at[2], from_x.at[1])
    yl.start()
    swaps[3].wait_recv()
    loads[3].wait()
    xl.wait_recv()
    yh.wait_recv()
    xh.wait_recv()
    yl.wait_recv()
    add(o_ref, 0, rows, mine.at[3], from_core.at[3], from_x.at[0], from_y.at[0])
    for s in (*swaps, dx, dy, xl, xh, yl, yh):
        s.wait_send()

def scatter_sum(p, ident, dtype=jnp.float32):
    rows, width = p.shape[0] // 8, p.shape[1]
    low = jnp.bfloat16
    return pl.pallas_call(
        functools.partial(scatter_kernel, rows),
        out_shape=jax.ShapeDtypeStruct((rows, width), dtype),
        in_specs=[pl.BlockSpec(memory_space=pl.ANY)],
        out_specs=pl.BlockSpec(memory_space=pltpu.VMEM),
        scratch_shapes=[
            pltpu.VMEM((4, rows, width), low), pltpu.VMEM((4, rows, width), low),
            pltpu.VMEM((3, rows, width), low), pltpu.VMEM((2, rows, width), low),
            pltpu.VMEM((2, rows, width), low),
            pltpu.SemaphoreType.DMA((10,)), pltpu.SemaphoreType.DMA((10,)), pltpu.SemaphoreType.DMA((4,))],
        compiler_params=pltpu.CompilerParams(collective_id=ident, has_side_effects=True, vmem_limit_bytes=40 << 20),
    )(p)


def vector_kernel(v_ref, o_ref, got, total, far, send, recv):
    me, c, x, y, at = positions()
    z = lax.axis_index("dp")
    count = lax.axis_size("dp")
    pairs = (at(y, x, 1 - c), at(y, 1 - x, c), at(1 - y, x, c))
    others = [lax.rem(z + k, count) for k in range(1, count)]
    barrier = pltpu.get_barrier_semaphore()
    for peer in pairs:
        pl.semaphore_signal(barrier, inc=1, device_id={"tensor": peer}, device_id_type=MESH)
    for peer in others:
        pl.semaphore_signal(barrier, inc=1, device_id={"dp": peer}, device_id_type=MESH)
    pl.semaphore_wait(barrier, len(pairs) + len(others))
    everyone = 6
    total[...] = v_ref[...]
    for k, peer in enumerate(pairs):
        swap = pltpu.make_async_remote_copy(
            src_ref=total, dst_ref=got.at[k], send_sem=send.at[k], recv_sem=recv.at[k],
            device_id={"tensor": peer}, device_id_type=MESH)
        swap.start()
        swap.wait()
        total[:everyone, :] = total[:everyone, :] + got[k, :everyone, :]
    far[z] = total[...]
    swaps = []
    for k, peer in enumerate(others):
        swaps.append(pltpu.make_async_remote_copy(
            src_ref=total, dst_ref=far.at[z], send_sem=send.at[3 + k], recv_sem=recv.at[3 + k],
            device_id={"dp": peer}, device_id_type=MESH))
    for swap in swaps:
        swap.start()
    for swap in swaps:
        swap.wait()
    acc = far[0]
    for k in range(1, count):
        acc = acc + far[k]
    o_ref[...] = acc


def vector_sum(v):
    count = lax.axis_size("dp")
    return pl.pallas_call(
        vector_kernel,
        out_shape=jax.ShapeDtypeStruct(v.shape, v.dtype),
        in_specs=[pl.BlockSpec(memory_space=pltpu.VMEM)],
        out_specs=pl.BlockSpec(memory_space=pltpu.VMEM),
        scratch_shapes=[
            pltpu.VMEM((3,) + v.shape, v.dtype),
            pltpu.VMEM(v.shape, v.dtype),
            pltpu.VMEM((count,) + v.shape, v.dtype),
            pltpu.SemaphoreType.DMA((3 + count - 1,)),
            pltpu.SemaphoreType.DMA((3 + count - 1,)),
        ],
        compiler_params=pltpu.CompilerParams(collective_id=3, has_side_effects=True),
    )(v)


def nt_dot(left, right):
    return lax.dot_general(left, right, (((1,), (1,)), ((), ())), preferred_element_type=jnp.float32)


def nn_dot(left, right):
    return jnp.dot(left, right, preferred_element_type=jnp.float32)


def first_positions(lengths_ref, row, base, count):
    places = base + lax.broadcasted_iota(jnp.int32, (1, count), 1)
    begin = jnp.int32(0)
    first = jnp.zeros((1, count), jnp.int32)
    for doc in range(lengths_ref.shape[1] - 1):
        begin = begin + lengths_ref[row, doc]
        first = jnp.where(places >= begin, begin, first)
    return places, first


def masked_scores(lengths_ref, query_rows, key_rows, first_key, first_query):
    keys, queries = key_rows.shape[0], query_rows.shape[0]
    scores = nt_dot(key_rows, query_rows) * HD ** (-0.5)
    places, first = first_positions(lengths_ref, pl.program_id(0), first_query, queries)
    key_places = first_key + lax.broadcasted_iota(jnp.int32, (keys, queries), 0)
    allowed = (key_places >= first) & (key_places <= places)
    return scores, allowed


def attend_kernel(lengths_ref, joined_ref, out_ref, log_ref):
    length, width = out_ref.shape
    for head in range(width // HD):
        cols = slice(head * HD, (head + 1) * HD)
        value_t = joined_ref[2, :, cols].T
        for block in range(length // QUERY_BLOCK):
            first, stop = block * QUERY_BLOCK, (block + 1) * QUERY_BLOCK
            start = max(0, first - MOST_DOC)
            scores, allowed = masked_scores(
                lengths_ref, joined_ref[0, first:stop, cols], joined_ref[1, start:stop, cols], start, first)
            scores = jnp.where(allowed, scores, -1000000000.0)
            row_max = jnp.max(scores, axis=0, keepdims=True)
            exp_scores = jnp.exp(scores - row_max)
            row_total = jnp.sum(exp_scores, axis=0, keepdims=True)
            prob_low = (exp_scores * (1.0 / row_total)).astype(LOW)
            out_ref[first:stop, cols] = nn_dot(value_t[:, start:stop], prob_low).T.astype(LOW)
            log_ref[head : head + 1, first:stop] = row_max + jnp.log(row_total)


def attend(lengths, joined):
    rows = lengths.shape[0]
    tokens, width = joined.shape[1], joined.shape[2]
    length, heads = tokens // rows, width // HD
    area = rows * heads * length * MOST_DOC
    return pl.pallas_call(
        attend_kernel,
        grid=(rows,),
        out_shape=(
            jax.ShapeDtypeStruct((tokens, width), LOW),
            jax.ShapeDtypeStruct((rows, heads, length), jnp.float32),
        ),
        in_specs=[
            pl.BlockSpec(memory_space=pltpu.SMEM),
            pl.BlockSpec((3, length, width), lambda row: (0, row, 0)),
        ],
        out_specs=(
            pl.BlockSpec((length, width), lambda row: (row, 0)),
            pl.BlockSpec((None, heads, length), lambda row: (row, 0, 0)),
        ),
        compiler_params=pltpu.CompilerParams(vmem_limit_bytes=40 << 20),
        cost_estimate=pl.CostEstimate(flops=4 * area * HD, bytes_accessed=8 * tokens * width, transcendentals=area),
    )(lengths, joined)


def attend_back_kernel(lengths_ref, joined_ref, mixed_ref, log_ref, out_ref, sum_ref, key_acc, value_acc):
    length, width = mixed_ref.shape
    scale = HD ** (-0.5)
    for head in range(width // HD):
        cols = slice(head * HD, (head + 1) * HD)
        key_t = joined_ref[1, :, cols].T
        key_acc[...] = jnp.zeros_like(key_acc)
        value_acc[...] = jnp.zeros_like(value_acc)
        query_total = jnp.zeros((1, HD), jnp.float32)
        for block in range(length // QUERY_BLOCK):
            first, stop = block * QUERY_BLOCK, (block + 1) * QUERY_BLOCK
            start = max(0, first - MOST_DOC)
            query_rows = joined_ref[0, first:stop, cols]
            mixed_rows = mixed_ref[first:stop, cols]
            scores, allowed = masked_scores(
                lengths_ref, query_rows, joined_ref[1, start:stop, cols], start, first)
            prob = jnp.where(allowed, jnp.exp(scores - log_ref[head : head + 1, first:stop]), 0.0)
            prob_grad = nt_dot(joined_ref[2, start:stop, cols], mixed_rows)
            inner = jnp.sum(prob * prob_grad, axis=0, keepdims=True)
            score_grad = (prob * (prob_grad - inner)).astype(LOW)
            query_grad = (nn_dot(key_t[:, start:stop], score_grad) * scale).T.astype(LOW)
            out_ref[0, first:stop, cols] = query_grad
            query_total = query_total + jnp.sum(query_grad.astype(jnp.float32), axis=0, keepdims=True)
            key_acc[start:stop, :] += nn_dot(score_grad, query_rows)
            value_acc[start:stop, :] += nn_dot(prob.astype(LOW), mixed_rows)
        value_grad = value_acc[...].astype(LOW)
        out_ref[1, :, cols] = (key_acc[...] * scale).astype(LOW)
        out_ref[2, :, cols] = value_grad
        sum_ref[0:1, cols] = query_total
        sum_ref[1:2, cols] = jnp.sum(value_grad.astype(jnp.float32), axis=0, keepdims=True)


def attend_back(lengths, joined, mixed_grad, log_total):
    rows = lengths.shape[0]
    tokens, width = mixed_grad.shape
    length, heads = tokens // rows, width // HD
    area = rows * heads * length * MOST_DOC
    return pl.pallas_call(
        attend_back_kernel,
        grid=(rows,),
        out_shape=(
            jax.ShapeDtypeStruct((3, tokens, width), LOW),
            jax.ShapeDtypeStruct((rows, 2, width), jnp.float32),
        ),
        in_specs=[
            pl.BlockSpec(memory_space=pltpu.SMEM),
            pl.BlockSpec((3, length, width), lambda row: (0, row, 0)),
            pl.BlockSpec((length, width), lambda row: (row, 0)),
            pl.BlockSpec((None, heads, length), lambda row: (row, 0, 0)),
        ],
        out_specs=(
            pl.BlockSpec((3, length, width), lambda row: (0, row, 0)),
            pl.BlockSpec((None, 2, width), lambda row: (row, 0, 0)),
        ),
        scratch_shapes=[pltpu.VMEM((length, HD), jnp.float32), pltpu.VMEM((length, HD), jnp.float32)],
        compiler_params=pltpu.CompilerParams(vmem_limit_bytes=40 << 20),
        cost_estimate=pl.CostEstimate(flops=10 * area * HD, bytes_accessed=16 * tokens * width, transcendentals=area),
    )(lengths, joined, mixed_grad, log_total)


def standardize(values):
    centred = values - jnp.mean(values, axis=-1, keepdims=True)
    inverse = lax.rsqrt(jnp.mean(centred * centred, axis=-1, keepdims=True) + NORM_EPS)
    return centred * inverse, inverse


def norm_back(unit, inverse, grad, gain):
    scaled = grad * gain
    inner = jnp.mean(scaled * unit, axis=-1, keepdims=True)
    part = (scaled - jnp.mean(scaled, axis=-1, keepdims=True) - unit * inner) * inverse
    return part, jnp.sum(grad * unit, axis=0), jnp.sum(grad, axis=0)


def contract_first(left_arr, right_arr):
    return lax.dot_general(
        left_arr, right_arr, (((0,), (0,)), ((), ())), preferred_element_type=jnp.float32
    )


def line_sum(part):
    place = lax.axis_index("dp")
    outer = (place == 0) | (place == 3)
    inward = lax.ppermute(part, "dp", [(0, 1), (3, 2)])
    side = (part.astype(jnp.float32) + inward.astype(jnp.float32)).astype(LOW)
    side = lax.optimization_barrier(side)
    across = lax.ppermute(side, "dp", [(1, 2), (2, 1)])
    whole = (side.astype(jnp.float32) + across.astype(jnp.float32)).astype(LOW)
    whole = lax.optimization_barrier(whole)
    outward = lax.ppermute(whole, "dp", [(1, 0), (2, 3)])
    return jnp.where(outer, outward, whole).astype(jnp.float32)


def shards(
    inputs,
    doc_lengths,
    attn_gain,
    attn_shift,
    qkv_weight,
    qv_bias,
    out_weight,
    out_bias,
    mlp_gain,
    mlp_shift,
    up_weight,
    up_bias,
    down_weight,
    down_bias,
    out_grad,
):
    fast = lax.axis_size("tensor") == 8 and lax.axis_size("dp") == 4
    attn_gain32 = attn_gain.astype(jnp.float32)
    attn_shift32 = attn_shift.astype(jnp.float32)
    mlp_gain32 = mlp_gain.astype(jnp.float32)
    mlp_shift32 = mlp_shift.astype(jnp.float32)
    qkv = qkv_weight.transpose(1, 0, 2)

    def gather(block):
        if fast:
            return gather_rows(block, 1)
        return lax.all_gather(block, "tensor", axis=0, tiled=True)

    def scatter(partial):
        if fast:
            return scatter_sum(partial.astype(LOW), 2)
        return lax.psum_scatter(partial, "tensor", scatter_dimension=0, tiled=True)

    def side_scatter(partial):
        return lax.psum_scatter(
            partial.astype(LOW), "tensor", scatter_dimension=0, tiled=True
        ).astype(jnp.float32)

    def groups_sum(pieces):
        if fast:
            return [line_sum(piece.astype(LOW)) for piece in pieces]
        return [lax.psum(piece, "dp") for piece in pieces]

    inputs32 = inputs.astype(jnp.float32)
    attn_unit, attn_inverse = standardize(inputs32)
    attn_rows = gather((attn_unit * attn_gain32 + attn_shift32).astype(LOW))
    late_grad, attn_rows = lax.optimization_barrier((out_grad, attn_rows))
    grad_rows = lax.all_gather(late_grad, "tensor", axis=0, tiled=True)
    bias = jnp.stack([qv_bias[0], jnp.zeros_like(qv_bias[0]), qv_bias[1]]).astype(jnp.float32)
    joined = jnp.einsum("td,cdh->cth", attn_rows, qkv, preferred_element_type=jnp.float32)
    joined = (joined + bias[:, None, :]).astype(LOW)
    heads_out, log_total = attend(doc_lengths, joined)
    attn_sum = scatter(nn_dot(heads_out, out_weight))
    middle = inputs32 + attn_sum + out_bias
    mlp_unit, mlp_inverse = standardize(middle)
    mlp_rows = gather((mlp_unit * mlp_gain32 + mlp_shift32).astype(LOW))
    pre_act = nn_dot(mlp_rows, up_weight) + up_bias
    hidden, gelu_pull = jax.vjp(lambda value_in: jax.nn.gelu(value_in, approximate=True), pre_act)
    hidden = hidden.astype(LOW)
    half = hidden.shape[1] // 2
    down_grads = groups_sum([contract_first(hidden[:, :half], grad_rows), contract_first(hidden[:, half:], grad_rows)])
    hidden_grad = lax.dot_general(
        grad_rows, down_weight, (((1,), (1,)), ((), ())), preferred_element_type=jnp.float32
    )
    pre_grad = gelu_pull(hidden_grad)[0].astype(LOW)
    up_bias_grad = jnp.sum(pre_grad, axis=0, dtype=jnp.float32)
    width = mlp_rows.shape[1] // 2
    up_grads = groups_sum([contract_first(mlp_rows[:, :width], pre_grad), contract_first(mlp_rows[:, width:], pre_grad)])
    mlp_sum = side_scatter(nn_dot(hidden, down_weight))
    outputs = (middle + mlp_sum + down_bias).astype(LOW)
    grad32 = out_grad.astype(jnp.float32)
    down_bias_grad = jnp.sum(grad32, axis=0)
    mlp_norm_grad = scatter(nt_dot(pre_grad, up_weight))
    middle_part, mlp_gain_grad, mlp_shift_grad = norm_back(mlp_unit, mlp_inverse, mlp_norm_grad, mlp_gain32)
    middle_grad = grad32 + middle_part
    out_bias_grad = jnp.sum(middle_grad, axis=0)
    middle_rows = gather(middle_grad.astype(LOW))
    mixed_grad = nt_dot(middle_rows, out_weight).astype(LOW)
    out_grads = groups_sum([contract_first(heads_out, middle_rows)])
    joined_grad, bias_sums = attend_back(doc_lengths, joined, mixed_grad, log_total)
    qkv_grads = groups_sum([contract_first(attn_rows, joined_grad[part]) for part in range(3)])
    attn_norm_grad = scatter(
        jnp.einsum("cth,cdh->td", joined_grad, qkv, preferred_element_type=jnp.float32)
    )
    input_part, attn_gain_grad, attn_shift_grad = norm_back(attn_unit, attn_inverse, attn_norm_grad, attn_gain32)
    input_grad = middle_grad + input_part
    qv_bias_grad = jnp.sum(bias_sums, axis=0)
    shared = [attn_gain_grad, attn_shift_grad, out_bias_grad, mlp_gain_grad, mlp_shift_grad, down_bias_grad]
    if fast:
        own = jnp.concatenate([up_bias_grad, qv_bias_grad.reshape(-1)])
        own = jnp.pad(own, (0, 2 * shared[0].shape[0] - own.shape[0])).reshape(2, -1)
        summed = vector_sum(jnp.concatenate([jnp.stack(shared), own]))
        shared = [summed[index] for index in range(6)]
        own = summed[6:].reshape(-1)
        up_bias_grad = own[: up_bias_grad.shape[0]]
        qv_bias_grad = own[up_bias_grad.shape[0] :][: qv_bias_grad.size].reshape(qv_bias_grad.shape)
    else:
        shared = lax.psum(shared, ("dp", "tensor"))
        up_bias_grad, qv_bias_grad = lax.psum((up_bias_grad, qv_bias_grad), "dp")
    return (
        outputs,
        input_grad,
        shared[0],
        shared[1],
        jnp.stack(qkv_grads).transpose(1, 0, 2),
        qv_bias_grad,
        out_grads[0],
        shared[2],
        shared[3],
        shared[4],
        jnp.concatenate(up_grads),
        up_bias_grad,
        jnp.concatenate(down_grads),
        shared[5],
    )


def solution(mesh):
    return jax.shard_map(
        shards,
        mesh=mesh,
        in_specs=(
            P(("dp", "tensor"), None),
            P("dp", None),
            P(),
            P(),
            P(None, None, "tensor"),
            P(None, "tensor"),
            P("tensor", None),
            P(),
            P(),
            P(),
            P(None, "tensor"),
            P("tensor"),
            P("tensor", None),
            P(),
            P(("dp", "tensor"), None),
        ),
        out_specs=(
            P(("dp", "tensor"), None),
            P(("dp", "tensor"), None),
            P(),
            P(),
            P(None, None, "tensor"),
            P(None, "tensor"),
            P("tensor", None),
            P(),
            P(),
            P(),
            P(None, "tensor"),
            P("tensor"),
            P("tensor", None),
            P(),
        ),
        check_vma=False,
    )
```

```python
import functools

import jax
import jax.numpy as jnp
from jax import lax
from jax.experimental import pallas as pl
from jax.experimental.pallas import tpu as pltpu
from jax.sharding import PartitionSpec as P

HD = 128
MOST_DOC = 512
QUERY_BLOCK = 256
NORM_EPS = 1e-05
LOW = jnp.bfloat16
MESH = pl.DeviceIdType.MESH
LINK_COST = pl.CostEstimate(flops=0, bytes_accessed=140 << 20, transcendentals=0)


def positions():
    me = lax.axis_index("tensor")
    core = me % 2
    col = (me // 2) % 2
    row = me // 4
    def at(r, x, c):
        return r * 4 + x * 2 + c
    return me, core, col, row, at

def greet(peers):
    barrier = pltpu.get_barrier_semaphore()
    for peer in peers:
        pl.semaphore_signal(barrier, inc=1, device_id={"tensor": peer}, device_id_type=MESH)
    pl.semaphore_wait(barrier, len(peers))

def gather_kernel(rows, x_ref, o_ref, send, recv, local):
    me, c, x, y, at = positions()
    tx, ty, tc = at(y, 1 - x, c), at(1 - y, x, c), at(y, x, 1 - c)
    td = at(1 - y, 1 - x, c)
    txc, tyc, tdc = at(y, 1 - x, 1 - c), at(1 - y, x, 1 - c), at(1 - y, 1 - x, 1 - c)
    half = rows // 2
    greet((tx, ty, tc))

    def place(block, part):
        return o_ref.at[pl.ds(pl.multiple_of(block * rows + part * half, half), half), :]

    def copy(src, block, part, index, peer):
        return pltpu.make_async_remote_copy(
            src_ref=src, dst_ref=place(block, part), send_sem=send.at[index],
            recv_sem=recv.at[index], device_id={"tensor": peer}, device_id_type=MESH)

    def own(part):
        return x_ref.at[pl.ds(part * half, half), :]

    keep = pltpu.make_async_copy(x_ref, o_ref.at[pl.ds(pl.multiple_of(me * rows, rows), rows), :], local)
    sx0 = copy(own(0), me, 0, 0, tx)
    sy1 = copy(own(1), me, 1, 1, ty)
    sx1 = copy(own(1), me, 1, 2, tx)
    sy0 = copy(own(0), me, 0, 3, ty)
    sc0 = copy(own(0), me, 0, 4, tc)
    sc1 = copy(own(1), me, 1, 5, tc)
    for s in (sx0, sy1, sx1, sy0, sc0, sc1):
        s.start()
    keep.start()
    fy = copy(place(tx, 0), tx, 0, 6, ty)
    fx = copy(place(ty, 1), ty, 1, 7, tx)
    cx0 = copy(place(tx, 0), tx, 0, 8, tc)
    cy1 = copy(place(ty, 1), ty, 1, 9, tc)
    cx1 = copy(place(tx, 1), tx, 1, 10, tc)
    cy0 = copy(place(ty, 0), ty, 0, 11, tc)
    cd0 = copy(place(td, 0), td, 0, 12, tc)
    cd1 = copy(place(td, 1), td, 1, 13, tc)
    sx0.wait_recv()
    fy.start()
    cx0.start()
    sy1.wait_recv()
    fx.start()
    cy1.start()
    sx1.wait_recv()
    cx1.start()
    sy0.wait_recv()
    cy0.start()
    fy.wait_recv()
    cd0.start()
    fx.wait_recv()
    cd1.start()
    for s in (sc0, sc1, cx0, cy1, cx1, cy0, cd0, cd1):
        s.wait_recv()
    for s in (sx0, sy1, sx1, sy0, sc0, sc1, fy, fx, cx0, cy1, cx1, cy0, cd0, cd1):
        s.wait_send()
    keep.wait()

def gather_rows(x, ident):
    rows, width = x.shape
    return pl.pallas_call(
        functools.partial(gather_kernel, rows),
        out_shape=jax.ShapeDtypeStruct((8 * rows, width), x.dtype),
        in_specs=[pl.BlockSpec(memory_space=pl.ANY)],
        out_specs=pl.BlockSpec(memory_space=pl.ANY),
        scratch_shapes=[pltpu.SemaphoreType.DMA((14,)), pltpu.SemaphoreType.DMA((14,)), pltpu.SemaphoreType.DMA],
        compiler_params=pltpu.CompilerParams(collective_id=ident, has_side_effects=True),
        cost_estimate=LINK_COST,
    )(x)

TILE = 32


def add_into(dst, start, size, *srcs):
    @pl.loop(0, size // TILE)
    def _(step):
        rows = pl.ds(pl.multiple_of(start + step * TILE, TILE), TILE)
        acc = srcs[0][rows, :].astype(jnp.float32)
        for src in srcs[1:]:
            acc = acc + src[rows, :].astype(jnp.float32)
        dst[rows, :] = acc.astype(dst.dtype)


def scatter_steps(rows, p_ref, o_ref, mine, from_core, from_x, from_y, send, recv, local):
    me, c, x, y, at = positions()
    tx, ty, tc = at(y, 1 - x, c), at(1 - y, x, c), at(y, x, 1 - c)
    half = rows // 2
    chips = ((1 - y, 1 - x), (y, 1 - x), (1 - y, x), (y, x))

    def block(r, xx, cc):
        return p_ref.at[pl.ds(pl.multiple_of(at(r, xx, cc) * rows, rows), rows), :]

    def remote(src, dst, index, peer):
        return pltpu.make_async_remote_copy(
            src_ref=src, dst_ref=dst, send_sem=send.at[index],
            recv_sem=recv.at[index], device_id={"tensor": peer}, device_id_type=MESH)

    swaps = [remote(block(*chips[k], 1 - c), from_core.at[k], k, tc) for k in range(4)]
    loads = [pltpu.make_async_copy(block(*chips[k], c), mine.at[k], local.at[k]) for k in range(4)]
    for k in range(4):
        swaps[k].start()
        loads[k].start()

    lo, hi = pl.ds(0, half), pl.ds(half, half)
    dx = remote(mine.at[0, lo, :], from_x.at[1, lo, :], 4, tx)
    dy = remote(mine.at[0, hi, :], from_y.at[1, hi, :], 5, ty)
    xl = remote(mine.at[1, lo, :], from_x.at[0, lo, :], 6, tx)
    xh = remote(mine.at[1, hi, :], from_x.at[0, hi, :], 7, tx)
    yl = remote(mine.at[2, lo, :], from_y.at[0, lo, :], 8, ty)
    yh = remote(mine.at[2, hi, :], from_y.at[0, hi, :], 9, ty)

    swaps[0].wait_recv()
    loads[0].wait()
    add_into(mine.at[0], 0, half, mine.at[0], from_core.at[0])
    dx.start()
    add_into(mine.at[0], half, half, mine.at[0], from_core.at[0])
    dy.start()
    yield
    swaps[1].wait_recv()
    loads[1].wait()
    add_into(mine.at[1], 0, half, mine.at[1], from_core.at[1])
    xl.start()
    swaps[2].wait_recv()
    loads[2].wait()
    add_into(mine.at[2], half, half, mine.at[2], from_core.at[2])
    yh.start()
    yield
    dy.wait_recv()
    add_into(mine.at[1], half, half, mine.at[1], from_core.at[1], from_y.at[1])
    xh.start()
    dx.wait_recv()
    add_into(mine.at[2], 0, half, mine.at[2], from_core.at[2], from_x.at[1])
    yl.start()
    yield
    swaps[3].wait_recv()
    loads[3].wait()
    xl.wait_recv()
    yh.wait_recv()
    yield
    xh.wait_recv()
    yl.wait_recv()
    add_into(o_ref, 0, rows, mine.at[3], from_core.at[3], from_x.at[0], from_y.at[0])
    for s in (*swaps, dx, dy, xl, xh, yl, yh):
        s.wait_send()


def scatter_kernel(rows, *refs):
    me, c, x, y, at = positions()
    greet((at(y, 1 - x, c), at(1 - y, x, c), at(y, x, 1 - c)))
    for _ in scatter_steps(rows, *refs):
        pass


def scatter_scratch(rows, width):
    return [
        pltpu.VMEM((4, rows, width), LOW), pltpu.VMEM((4, rows, width), LOW),
        pltpu.VMEM((2, rows, width), LOW), pltpu.VMEM((2, rows, width), LOW),
        pltpu.SemaphoreType.DMA((10,)), pltpu.SemaphoreType.DMA((10,)), pltpu.SemaphoreType.DMA((4,))]


def scatter_sum(p, ident, dtype=jnp.float32):
    rows, width = p.shape[0] // 8, p.shape[1]
    return pl.pallas_call(
        functools.partial(scatter_kernel, rows),
        out_shape=jax.ShapeDtypeStruct((rows, width), dtype),
        in_specs=[pl.BlockSpec(memory_space=pl.ANY)],
        out_specs=pl.BlockSpec(memory_space=pltpu.VMEM),
        scratch_shapes=scatter_scratch(rows, width),
        compiler_params=pltpu.CompilerParams(collective_id=ident, has_side_effects=True, vmem_limit_bytes=40 << 20),
        cost_estimate=LINK_COST,
    )(p)


def line_steps(chunks, load, inward, across, outward, keep):
    place = lax.axis_index("dp")
    outer = lax.rem(place, 3) == 0
    inner = lax.rem(place, 3) != 0
    near, beside, end = 1 + place // 3, 3 - place, (place - 1) * 3

    def remote(src, dst, sems, index, peer):
        return pltpu.make_async_remote_copy(
            src_ref=src, dst_ref=dst, send_sem=sems.at[0, index], recv_sem=sems.at[1, index],
            device_id={"dp": peer}, device_id_type=MESH)

    first = [remote(part, got, inward, k, near) for k, (part, own, got, cross, out) in enumerate(chunks)]
    second = [remote(own, cross, across, k, beside) for k, (part, own, got, cross, out) in enumerate(chunks)]
    third = [remote(cross, out, outward, k, end) for k, (part, own, got, cross, out) in enumerate(chunks)]
    loads = [pltpu.make_async_copy(part, own, load.at[k]) for k, (part, own, got, cross, out) in enumerate(chunks)]
    keeps = [pltpu.make_async_copy(cross, out, keep.at[k]) for k, (part, own, got, cross, out) in enumerate(chunks)]
    count = len(chunks)

    @pl.when(inner)
    def _():
        for copy in loads:
            copy.start()

    for step in range(count + 3):
        @pl.when(outer)
        def _(step=step):
            if 2 <= step < count + 2:
                first[step - 2].wait_send()
            if step < count:
                first[step].start()

        @pl.when(inner)
        def _(step=step):
            k = step - 1
            if 0 <= k < count:
                loads[k].wait()
                first[k].wait_recv()
                part, own, got, cross, out = chunks[k]
                add_into(own, 0, own.shape[0], own, got)
                second[k].start()
            k = step - 2
            if 0 <= k < count:
                second[k].wait_recv()
                part, own, got, cross, out = chunks[k]
                add_into(cross, 0, own.shape[0], own, cross)
                third[k].start()
                keeps[k].start()
        yield

    @pl.when(outer)
    def _():
        for copy in third:
            copy.wait_recv()

    @pl.when(inner)
    def _():
        for k in range(count):
            second[k].wait_send()
            third[k].wait_send()
            keeps[k].wait()


def line_chunks(parts, own, got, cross, outs):
    chunks = []
    for part, a, b, c, out in zip(parts, own, got, cross, outs):
        if len(part.shape) == 3:
            half = part.shape[1] // 2
            views = [(lead, pl.ds(first, half), slice(None)) for lead in range(part.shape[0]) for first in (0, half)]
        else:
            size = (1 << 18) // part.shape[1]
            views = [(pl.ds(first, size), slice(None)) for first in range(0, part.shape[0], size)]
        for view in views:
            chunks.append(tuple(ref.at[view] for ref in (part, a, b, c, out)))
    return chunks


def greet_all():
    me, c, x, y, at = positions()
    place = lax.axis_index("dp")
    barrier = pltpu.get_barrier_semaphore()
    for peer in (at(y, 1 - x, c), at(1 - y, x, c), at(y, x, 1 - c)):
        pl.semaphore_signal(barrier, inc=1, device_id={"tensor": peer}, device_id_type=MESH)

    @pl.when(lax.rem(place, 3) == 0)
    def _():
        pl.semaphore_signal(barrier, inc=1, device_id={"dp": 1 + place // 3}, device_id_type=MESH)
        pl.semaphore_wait(barrier, 4)

    @pl.when(lax.rem(place, 3) != 0)
    def _():
        pl.semaphore_signal(barrier, inc=1, device_id={"dp": 3 - place}, device_id_type=MESH)
        pl.semaphore_signal(barrier, inc=1, device_id={"dp": (place - 1) * 3}, device_id_type=MESH)
        pl.semaphore_wait(barrier, 5)


def closing_kernel(rows, amount, *refs):
    p_ref, late_ref, parts = refs[0], refs[1], refs[2 : 2 + amount]
    refs = refs[2 + amount :]
    o_ref, late_out, outs = refs[0], refs[1], refs[2 : 2 + amount]
    rest = refs[2 + amount :]
    own, got, cross = rest[:amount], rest[amount : 2 * amount], rest[2 * amount : 3 * amount]
    load, inward, across, outward, keep = rest[3 * amount : 3 * amount + 5]
    scatter_refs = rest[3 * amount + 5 :]
    greet_all()
    line = line_steps(line_chunks(parts, own, got, cross, outs), load, inward, across, outward, keep)
    next(line)
    for _ in scatter_steps(rows, p_ref, o_ref, *scatter_refs[:7]):
        next(line)
    for _ in scatter_steps(rows, late_ref, late_out, *scatter_refs[7:]):
        next(line)
    for _ in line:
        pass


def closing_sums(p, late, parts, ident):
    rows, width = p.shape[0] // 8, p.shape[1]
    amount = len(parts)
    count = sum(part.size for part in parts) >> 18
    anywhere = pl.BlockSpec(memory_space=pl.ANY)
    inside = pl.BlockSpec(memory_space=pltpu.VMEM)
    boxes = [pltpu.VMEM(part.shape, LOW) for part in parts]
    pairs = pltpu.SemaphoreType.DMA((2, count))
    single = pltpu.SemaphoreType.DMA((count,))
    return pl.pallas_call(
        functools.partial(closing_kernel, rows, amount),
        out_shape=(jax.ShapeDtypeStruct((rows, width), jnp.float32),) * 2
        + tuple(jax.ShapeDtypeStruct(part.shape, LOW) for part in parts),
        in_specs=[anywhere] * (2 + amount),
        out_specs=(inside, inside) + (anywhere,) * amount,
        scratch_shapes=boxes * 3 + [single, pairs, pairs, pairs, single] + scatter_scratch(rows, width) * 2,
        compiler_params=pltpu.CompilerParams(collective_id=ident, has_side_effects=True, vmem_limit_bytes=58 << 20),
        cost_estimate=LINK_COST,
    )(p, late, *parts)


def vector_kernel(v_ref, o_ref, got, total, far, send, recv):
    me, c, x, y, at = positions()
    z = lax.axis_index("dp")
    count = lax.axis_size("dp")
    pairs = (at(y, x, 1 - c), at(y, 1 - x, c), at(1 - y, x, c))
    others = [lax.rem(z + k, count) for k in range(1, count)]
    barrier = pltpu.get_barrier_semaphore()
    for peer in pairs:
        pl.semaphore_signal(barrier, inc=1, device_id={"tensor": peer}, device_id_type=MESH)
    for peer in others:
        pl.semaphore_signal(barrier, inc=1, device_id={"dp": peer}, device_id_type=MESH)
    pl.semaphore_wait(barrier, len(pairs) + len(others))
    everyone = 6
    total[...] = v_ref[...]
    for k, peer in enumerate(pairs):
        swap = pltpu.make_async_remote_copy(
            src_ref=total, dst_ref=got.at[k], send_sem=send.at[k], recv_sem=recv.at[k],
            device_id={"tensor": peer}, device_id_type=MESH)
        swap.start()
        swap.wait()
        total[:everyone, :] = total[:everyone, :] + got[k, :everyone, :]
    far[z] = total[...]
    swaps = []
    for k, peer in enumerate(others):
        swaps.append(pltpu.make_async_remote_copy(
            src_ref=total, dst_ref=far.at[z], send_sem=send.at[3 + k], recv_sem=recv.at[3 + k],
            device_id={"dp": peer}, device_id_type=MESH))
    for swap in swaps:
        swap.start()
    for swap in swaps:
        swap.wait()
    acc = far[0]
    for k in range(1, count):
        acc = acc + far[k]
    o_ref[...] = acc


def vector_sum(v):
    count = lax.axis_size("dp")
    return pl.pallas_call(
        vector_kernel,
        out_shape=jax.ShapeDtypeStruct(v.shape, v.dtype),
        in_specs=[pl.BlockSpec(memory_space=pltpu.VMEM)],
        out_specs=pl.BlockSpec(memory_space=pltpu.VMEM),
        scratch_shapes=[
            pltpu.VMEM((3,) + v.shape, v.dtype),
            pltpu.VMEM(v.shape, v.dtype),
            pltpu.VMEM((count,) + v.shape, v.dtype),
            pltpu.SemaphoreType.DMA((3 + count - 1,)),
            pltpu.SemaphoreType.DMA((3 + count - 1,)),
        ],
        compiler_params=pltpu.CompilerParams(collective_id=3, has_side_effects=True),
    )(v)


def nt_dot(left, right):
    return lax.dot_general(left, right, (((1,), (1,)), ((), ())), preferred_element_type=jnp.float32)


def nn_dot(left, right):
    return jnp.dot(left, right, preferred_element_type=jnp.float32)


def first_positions(lengths_ref, row, base, count):
    places = base + lax.broadcasted_iota(jnp.int32, (1, count), 1)
    begin = jnp.int32(0)
    first = jnp.zeros((1, count), jnp.int32)
    for doc in range(lengths_ref.shape[1] - 1):
        begin = begin + lengths_ref[row, doc]
        first = jnp.where(places >= begin, begin, first)
    return places, first


def masked_scores(lengths_ref, query_rows, key_rows, first_key, first_query):
    keys, queries = key_rows.shape[0], query_rows.shape[0]
    scores = nt_dot(key_rows, query_rows) * HD ** (-0.5)
    places, first = first_positions(lengths_ref, pl.program_id(0), first_query, queries)
    key_places = first_key + lax.broadcasted_iota(jnp.int32, (keys, queries), 0)
    allowed = (key_places >= first) & (key_places <= places)
    return scores, allowed


def attend_kernel(lengths_ref, joined_ref, out_ref, log_ref):
    length, width = out_ref.shape
    for head in range(width // HD):
        cols = slice(head * HD, (head + 1) * HD)
        value_t = joined_ref[2, :, cols].T
        for block in range(length // QUERY_BLOCK):
            first, stop = block * QUERY_BLOCK, (block + 1) * QUERY_BLOCK
            start = max(0, first - MOST_DOC)
            scores, allowed = masked_scores(
                lengths_ref, joined_ref[0, first:stop, cols], joined_ref[1, start:stop, cols], start, first)
            scores = jnp.where(allowed, scores, -1000000000.0)
            row_max = jnp.max(scores, axis=0, keepdims=True)
            exp_scores = jnp.exp(scores - row_max)
            row_total = jnp.sum(exp_scores, axis=0, keepdims=True)
            prob_low = (exp_scores * (1.0 / row_total)).astype(LOW)
            out_ref[first:stop, cols] = nn_dot(value_t[:, start:stop], prob_low).T.astype(LOW)
            log_ref[head : head + 1, first:stop] = row_max + jnp.log(row_total)


def attend(lengths, joined):
    rows = lengths.shape[0]
    tokens, width = joined.shape[1], joined.shape[2]
    length, heads = tokens // rows, width // HD
    area = rows * heads * length * MOST_DOC
    return pl.pallas_call(
        attend_kernel,
        grid=(rows,),
        out_shape=(
            jax.ShapeDtypeStruct((tokens, width), LOW),
            jax.ShapeDtypeStruct((rows, heads, length), jnp.float32),
        ),
        in_specs=[
            pl.BlockSpec(memory_space=pltpu.SMEM),
            pl.BlockSpec((3, length, width), lambda row: (0, row, 0)),
        ],
        out_specs=(
            pl.BlockSpec((length, width), lambda row: (row, 0)),
            pl.BlockSpec((None, heads, length), lambda row: (row, 0, 0)),
        ),
        compiler_params=pltpu.CompilerParams(vmem_limit_bytes=40 << 20),
        cost_estimate=pl.CostEstimate(flops=4 * area * HD, bytes_accessed=8 * tokens * width, transcendentals=area),
    )(lengths, joined)


def attend_back_kernel(lengths_ref, joined_ref, mixed_ref, log_ref, out_ref, sum_ref, key_acc, value_acc):
    length, width = mixed_ref.shape
    scale = HD ** (-0.5)
    for head in range(width // HD):
        cols = slice(head * HD, (head + 1) * HD)
        key_t = joined_ref[1, :, cols].T
        key_acc[...] = jnp.zeros_like(key_acc)
        value_acc[...] = jnp.zeros_like(value_acc)
        query_total = jnp.zeros((1, HD), jnp.float32)
        for block in range(length // QUERY_BLOCK):
            first, stop = block * QUERY_BLOCK, (block + 1) * QUERY_BLOCK
            start = max(0, first - MOST_DOC)
            query_rows = joined_ref[0, first:stop, cols]
            mixed_rows = mixed_ref[first:stop, cols]
            scores, allowed = masked_scores(
                lengths_ref, query_rows, joined_ref[1, start:stop, cols], start, first)
            prob = jnp.where(allowed, jnp.exp(scores - log_ref[head : head + 1, first:stop]), 0.0)
            prob_grad = nt_dot(joined_ref[2, start:stop, cols], mixed_rows)
            inner = jnp.sum(prob * prob_grad, axis=0, keepdims=True)
            score_grad = (prob * (prob_grad - inner)).astype(LOW)
            query_grad = (nn_dot(key_t[:, start:stop], score_grad) * scale).T.astype(LOW)
            out_ref[0, first:stop, cols] = query_grad
            query_total = query_total + jnp.sum(query_grad.astype(jnp.float32), axis=0, keepdims=True)
            key_acc[start:stop, :] += nn_dot(score_grad, query_rows)
            value_acc[start:stop, :] += nn_dot(prob.astype(LOW), mixed_rows)
        value_grad = value_acc[...].astype(LOW)
        out_ref[1, :, cols] = (key_acc[...] * scale).astype(LOW)
        out_ref[2, :, cols] = value_grad
        sum_ref[0:1, cols] = query_total
        sum_ref[1:2, cols] = jnp.sum(value_grad.astype(jnp.float32), axis=0, keepdims=True)


def attend_back(lengths, joined, mixed_grad, log_total):
    rows = lengths.shape[0]
    tokens, width = mixed_grad.shape
    length, heads = tokens // rows, width // HD
    area = rows * heads * length * MOST_DOC
    return pl.pallas_call(
        attend_back_kernel,
        grid=(rows,),
        out_shape=(
            jax.ShapeDtypeStruct((3, tokens, width), LOW),
            jax.ShapeDtypeStruct((rows, 2, width), jnp.float32),
        ),
        in_specs=[
            pl.BlockSpec(memory_space=pltpu.SMEM),
            pl.BlockSpec((3, length, width), lambda row: (0, row, 0)),
            pl.BlockSpec((length, width), lambda row: (row, 0)),
            pl.BlockSpec((None, heads, length), lambda row: (row, 0, 0)),
        ],
        out_specs=(
            pl.BlockSpec((3, length, width), lambda row: (0, row, 0)),
            pl.BlockSpec((None, 2, width), lambda row: (row, 0, 0)),
        ),
        scratch_shapes=[pltpu.VMEM((length, HD), jnp.float32), pltpu.VMEM((length, HD), jnp.float32)],
        compiler_params=pltpu.CompilerParams(vmem_limit_bytes=40 << 20),
        cost_estimate=pl.CostEstimate(flops=10 * area * HD, bytes_accessed=16 * tokens * width, transcendentals=area),
    )(lengths, joined, mixed_grad, log_total)


def standardize(values):
    centred = values - jnp.mean(values, axis=-1, keepdims=True)
    inverse = lax.rsqrt(jnp.mean(centred * centred, axis=-1, keepdims=True) + NORM_EPS)
    return centred * inverse, inverse


def norm_back(unit, inverse, grad, gain):
    scaled = grad * gain
    inner = jnp.mean(scaled * unit, axis=-1, keepdims=True)
    part = (scaled - jnp.mean(scaled, axis=-1, keepdims=True) - unit * inner) * inverse
    return part, jnp.sum(grad * unit, axis=0), jnp.sum(grad, axis=0)


def contract_first(left_arr, right_arr):
    return lax.dot_general(
        left_arr, right_arr, (((0,), (0,)), ((), ())), preferred_element_type=jnp.float32
    )


def gelu_pair(value):
    rate = 0.7978845608028654
    inner = jnp.tanh(rate * (value + 0.044715 * value * value * value))
    slope = 0.5 * (1.0 + inner) + 0.5 * value * (1.0 - inner * inner) * rate * (1.0 + 0.134145 * value * value)
    return 0.5 * value * (1.0 + inner), slope


def after(value, *anchors):
    return lax.optimization_barrier((value,) + anchors)[0]


def shards(
    inputs,
    doc_lengths,
    attn_gain,
    attn_shift,
    qkv_weight,
    qv_bias,
    out_weight,
    out_bias,
    mlp_gain,
    mlp_shift,
    up_weight,
    up_bias,
    down_weight,
    down_bias,
    out_grad,
):
    fast = lax.axis_size("tensor") == 8 and lax.axis_size("dp") == 4
    attn_gain32 = attn_gain.astype(jnp.float32)
    attn_shift32 = attn_shift.astype(jnp.float32)
    mlp_gain32 = mlp_gain.astype(jnp.float32)
    mlp_shift32 = mlp_shift.astype(jnp.float32)
    qkv = qkv_weight.transpose(1, 0, 2)

    def gather(block):
        if fast:
            return gather_rows(block, 1)
        return lax.all_gather(block, "tensor", axis=0, tiled=True)

    def scatter(partial):
        if fast:
            return scatter_sum(partial.astype(LOW), 2)
        return lax.psum_scatter(partial, "tensor", scatter_dimension=0, tiled=True)

    def side_scatter(partial):
        return lax.psum_scatter(
            partial.astype(LOW), "tensor", scatter_dimension=0, tiled=True
        ).astype(jnp.float32)

    inputs32 = inputs.astype(jnp.float32)
    attn_unit, attn_inverse = standardize(inputs32)
    attn_rows = gather((attn_unit * attn_gain32 + attn_shift32).astype(LOW))
    late_grad, attn_rows = lax.optimization_barrier((out_grad, attn_rows))
    grad_rows = lax.all_gather(late_grad, "tensor", axis=0, tiled=True)
    bias = jnp.stack([qv_bias[0], jnp.zeros_like(qv_bias[0]), qv_bias[1]]).astype(jnp.float32)
    joined = jnp.einsum("td,cdh->cth", attn_rows, qkv, preferred_element_type=jnp.float32)
    joined = (joined + bias[:, None, :]).astype(LOW)
    heads_out, log_total = attend(doc_lengths, joined)
    attn_sum = scatter(nn_dot(heads_out, out_weight))
    middle = inputs32 + attn_sum + out_bias
    mlp_unit, mlp_inverse = standardize(middle)
    mlp_rows = gather((mlp_unit * mlp_gain32 + mlp_shift32).astype(LOW))
    pre_act = nn_dot(mlp_rows, up_weight) + up_bias
    hidden, slope = gelu_pair(pre_act)
    hidden, slope = lax.optimization_barrier((hidden.astype(LOW), slope.astype(LOW)))
    down_part = contract_first(hidden, grad_rows)
    if fast:
        down_sum = lax.psum(down_part.astype(LOW), "dp").astype(jnp.float32)
    hidden_grad = lax.dot_general(
        after(grad_rows, down_part), down_weight, (((1,), (1,)), ((), ())), preferred_element_type=jnp.float32
    )
    pre_grad = (hidden_grad * slope.astype(jnp.float32)).astype(LOW)
    up_bias_grad = jnp.sum(pre_grad, axis=0, dtype=jnp.float32)
    mlp_part = nn_dot(hidden, down_weight).astype(LOW)
    grad32 = out_grad.astype(jnp.float32)
    down_bias_grad = jnp.sum(grad32, axis=0)
    mlp_norm_grad = scatter(nt_dot(pre_grad, up_weight))
    up_part = contract_first(mlp_rows, pre_grad)
    middle_part, mlp_gain_grad, mlp_shift_grad = norm_back(mlp_unit, mlp_inverse, mlp_norm_grad, mlp_gain32)
    middle_grad = grad32 + middle_part
    out_bias_grad = jnp.sum(middle_grad, axis=0)
    middle_rows = gather(middle_grad.astype(LOW))
    mixed_grad = nt_dot(middle_rows, out_weight).astype(LOW)
    out_part = contract_first(heads_out, middle_rows)
    joined_grad, bias_sums = attend_back(doc_lengths, joined, mixed_grad, log_total)
    qkv_part = jnp.einsum("td,cth->cdh", attn_rows, joined_grad, preferred_element_type=jnp.float32)
    attn_part = jnp.einsum("cth,cdh->td", joined_grad, qkv, preferred_element_type=jnp.float32)
    if fast:
        attn_norm_grad, mlp_sum, up_sum, out_sum, qkv_sum = closing_sums(
            attn_part.astype(LOW), mlp_part, [up_part.astype(LOW), out_part.astype(LOW), qkv_part.astype(LOW)], 4
        )
        up_sum, out_sum, qkv_sum = (part.astype(jnp.float32) for part in (up_sum, out_sum, qkv_sum))
    else:
        attn_norm_grad = scatter(attn_part)
        mlp_sum = side_scatter(mlp_part)
    outputs = (middle + mlp_sum + down_bias).astype(LOW)
    input_part, attn_gain_grad, attn_shift_grad = norm_back(attn_unit, attn_inverse, attn_norm_grad, attn_gain32)
    input_grad = middle_grad + input_part
    qv_bias_grad = jnp.sum(bias_sums, axis=0)
    shared = [attn_gain_grad, attn_shift_grad, out_bias_grad, mlp_gain_grad, mlp_shift_grad, down_bias_grad]
    if fast:
        own = jnp.concatenate([up_bias_grad, qv_bias_grad.reshape(-1)])
        own = jnp.pad(own, (0, 2 * shared[0].shape[0] - own.shape[0])).reshape(2, -1)
        summed = vector_sum(jnp.concatenate([jnp.stack(shared), own]))
        shared = [summed[index] for index in range(6)]
        own = summed[6:].reshape(-1)
        up_bias_grad = own[: up_bias_grad.shape[0]]
        qv_bias_grad = own[up_bias_grad.shape[0] :][: qv_bias_grad.size].reshape(qv_bias_grad.shape)
    else:
        shared = lax.psum(shared, ("dp", "tensor"))
        up_bias_grad, qv_bias_grad = lax.psum((up_bias_grad, qv_bias_grad), "dp")
        down_sum, up_sum, out_sum, qkv_sum = lax.psum((down_part, up_part, out_part, qkv_part), "dp")
    return (
        outputs,
        input_grad,
        shared[0],
        shared[1],
        qkv_sum.transpose(1, 0, 2),
        qv_bias_grad,
        out_sum,
        shared[2],
        shared[3],
        shared[4],
        up_sum,
        up_bias_grad,
        down_sum,
        shared[5],
    )


def solution(mesh):
    return jax.shard_map(
        shards,
        mesh=mesh,
        in_specs=(
            P(("dp", "tensor"), None),
            P("dp", None),
            P(),
            P(),
            P(None, None, "tensor"),
            P(None, "tensor"),
            P("tensor", None),
            P(),
            P(),
            P(),
            P(None, "tensor"),
            P("tensor"),
            P("tensor", None),
            P(),
            P(("dp", "tensor"), None),
        ),
        out_specs=(
            P(("dp", "tensor"), None),
            P(("dp", "tensor"), None),
            P(),
            P(),
            P(None, None, "tensor"),
            P(None, "tensor"),
            P("tensor", None),
            P(),
            P(),
            P(),
            P(None, "tensor"),
            P("tensor"),
            P("tensor", None),
            P(),
        ),
        check_vma=False,
    )
```

```python
import functools

import jax
import jax.numpy as jnp
from jax import lax
from jax.experimental import pallas as pl
from jax.experimental.pallas import tpu as pltpu
from jax.sharding import PartitionSpec as P

HD = 128
MOST_DOC = 512
QUERY_BLOCK = 256
NORM_EPS = 1e-05
LOW = jnp.bfloat16
MESH = pl.DeviceIdType.MESH
LINK_COST = pl.CostEstimate(flops=0, bytes_accessed=140 << 20, transcendentals=0)
TILE = 32
HALF_MEGA = 1 << 17
INSIDE = pl.BlockSpec(memory_space=pltpu.VMEM)
ANYWHERE = pl.BlockSpec(memory_space=pl.ANY)


def nt_dot(left, right):
    return lax.dot_general(left, right, (((1,), (1,)), ((), ())), preferred_element_type=jnp.float32)


def nn_dot(left, right):
    return jnp.dot(left, right, preferred_element_type=jnp.float32)


def contract_first(left_arr, right_arr):
    return lax.dot_general(
        left_arr, right_arr, (((0,), (0,)), ((), ())), preferred_element_type=jnp.float32
    )


def positions():
    me = lax.axis_index("tensor")
    core = me % 2
    col = (me // 2) % 2
    row = me // 4

    def at(r, x, c):
        return r * 4 + x * 2 + c

    return me, core, col, row, at


def greet_tensor():
    me, c, x, y, at = positions()
    barrier = pltpu.get_barrier_semaphore()
    for peer in (at(y, 1 - x, c), at(1 - y, x, c), at(y, x, 1 - c)):
        pl.semaphore_signal(barrier, inc=1, device_id={"tensor": peer}, device_id_type=MESH)
    pl.semaphore_wait(barrier, 3)


def stretch(start, size):
    return pl.ds(pl.multiple_of(start, size), size)


def add_into(dst, start, size, *srcs):
    @pl.loop(0, size // TILE)
    def _(step):
        rows = pl.ds(pl.multiple_of(start + step * TILE, TILE), TILE)
        acc = srcs[0][rows, :].astype(jnp.float32)
        for src in srcs[1:]:
            acc = acc + src[rows, :].astype(jnp.float32)
        dst[rows, :] = acc.astype(dst.dtype)


def standardize(values):
    centred = values - jnp.mean(values, axis=-1, keepdims=True)
    inverse = lax.rsqrt(jnp.mean(centred * centred, axis=-1, keepdims=True) + NORM_EPS)
    return centred * inverse, inverse


def gelu_pair(value):
    rate = 0.7978845608028654
    inner = jnp.tanh(rate * (value + 0.044715 * value * value * value))
    slope = 0.5 * (1.0 + inner) + 0.5 * value * (1.0 - inner * inner) * rate * (1.0 + 0.134145 * value * value)
    return 0.5 * value * (1.0 + inner), slope


def gather_loop(rows, held, whole, send, recv, keep, work):
    me, c, x, y, at = positions()
    tx, ty, tc = at(y, 1 - x, c), at(1 - y, x, c), at(y, x, 1 - c)
    td = at(1 - y, 1 - x, c)
    half = rows // 2

    def place(block, part):
        return held.at[pl.ds(pl.multiple_of(block * rows + part * half, half), half), :]

    def copy(block, part, index, peer):
        return pltpu.make_async_remote_copy(
            src_ref=place(block, part), dst_ref=place(block, part), send_sem=send.at[index],
            recv_sem=recv.at[index], device_id={"tensor": peer}, device_id_type=MESH)

    sx0, sy1, sx1, sy0 = copy(me, 0, 0, tx), copy(me, 1, 1, ty), copy(me, 1, 2, tx), copy(me, 0, 3, ty)
    sc0, sc1 = copy(me, 0, 4, tc), copy(me, 1, 5, tc)
    fy, fx = copy(tx, 0, 6, ty), copy(ty, 1, 7, tx)
    cx0, cy1, cx1, cy0 = copy(tx, 0, 8, tc), copy(ty, 1, 9, tc), copy(tx, 1, 10, tc), copy(ty, 0, 11, tc)
    cd0, cd1 = copy(td, 0, 12, tc), copy(td, 1, 13, tc)

    for s in (sx0, sy1, sx1, sy0, sc0, sc1):
        s.start()

    @pl.loop(0, 4)
    def _(group):
        middle = group * (3 - group) // 2
        last = group // 3

        @pl.when(group == 0)
        def _():
            sc0.wait_recv()
            sc1.wait_recv()

        @pl.when(group == 1)
        def _():
            sx0.wait_recv()
            fy.start()
            cx0.start()
            sy1.wait_recv()
            fx.start()
            cy1.start()
            sx1.wait_recv()
            cx1.start()
            sy0.wait_recv()
            cy0.start()

        @pl.when(group == 2)
        def _():
            for s in (cx0, cy1, cx1, cy0):
                s.wait_recv()

        @pl.when(group == 3)
        def _():
            fy.wait_recv()
            cd0.start()
            fx.wait_recv()
            cd1.start()

        @pl.loop(0, 2)
        def _(i):
            @pl.when(last * i == 1)
            def _():
                cd0.wait_recv()
                cd1.wait_recv()

            flip_x = middle * (1 - i) + last
            flip_y = middle * i + last
            flip_c = (1 - middle) * i + middle * (group - 1)
            block = at(y + flip_y * (1 - 2 * y), x + flip_x * (1 - 2 * x), c + flip_c * (1 - 2 * c))
            span = stretch(block * rows, rows)
            pltpu.make_async_copy(held.at[span, :], whole.at[span, :], keep.at[group * 2 + i]).start()
            work(span)

    for s in (sx0, sy1, sx1, sy0, sc0, sc1, fy, fx, cx0, cy1, cx1, cy0, cd0, cd1):
        s.wait_send()
    for k in range(8):
        pltpu.make_async_copy(held.at[:rows, :], whole.at[:rows, :], keep.at[k]).wait()


def gather_scratch(rows, width):
    return [
        pltpu.VMEM((8 * rows, width), LOW),
        pltpu.SemaphoreType.DMA((14,)),
        pltpu.SemaphoreType.DMA((14,)),
        pltpu.SemaphoreType.DMA((8,)),
    ]


def norm_into(held, rows, x_ref, gain_ref, shift_ref):
    base = lax.axis_index("tensor") * rows

    @pl.loop(0, rows // TILE)
    def _(step):
        first = step * TILE
        unit, inverse = standardize(x_ref[stretch(first, TILE), :].astype(jnp.float32))
        held[pl.ds(pl.multiple_of(base + first, TILE), TILE), :] = (unit * gain_ref[...] + shift_ref[...]).astype(LOW)


def gather_project_kernel(x_ref, gain_ref, shift_ref, w_ref, b_ref, whole, out_ref, held, send, recv, keep):
    rows = x_ref.shape[0]
    norm_into(held, rows, x_ref, gain_ref, shift_ref)
    greet_tensor()

    def work(span):
        @pl.loop(0, 3)
        def _(part):
            out_ref[part, span, :] = (nn_dot(held[span, :], w_ref[part]) + b_ref[part]).astype(LOW)

    gather_loop(rows, held, whole, send, recv, keep, work)


def gather_project(x, gain, shift, w, b):
    rows, width = x.shape
    return pl.pallas_call(
        gather_project_kernel,
        out_shape=(
            jax.ShapeDtypeStruct((8 * rows, width), LOW),
            jax.ShapeDtypeStruct((3, 8 * rows, w.shape[2]), LOW),
        ),
        in_specs=[INSIDE] * 5,
        out_specs=(ANYWHERE, INSIDE),
        scratch_shapes=gather_scratch(rows, width),
        compiler_params=pltpu.CompilerParams(collective_id=1, has_side_effects=True, vmem_limit_bytes=48 << 20),
        cost_estimate=LINK_COST,
    )(x, gain, shift, w, b)


def gather_hidden_kernel(x_ref, gain_ref, shift_ref, w_ref, b_ref, whole, out_ref, slope_ref, held, send, recv, keep):
    rows = x_ref.shape[0]
    norm_into(held, rows, x_ref, gain_ref, shift_ref)
    greet_tensor()

    def work(span):
        @pl.loop(0, w_ref.shape[1] // 512)
        def _(tile):
            cols = stretch(tile * 512, 512)
            hidden, slope = gelu_pair(nn_dot(held[span, :], w_ref[:, cols]) + b_ref[:, cols])
            out_ref[span, cols] = hidden.astype(LOW)
            slope_ref[span, cols] = slope.astype(LOW)

    gather_loop(rows, held, whole, send, recv, keep, work)


def gather_hidden(x, gain, shift, w, b):
    rows, width = x.shape
    return pl.pallas_call(
        gather_hidden_kernel,
        out_shape=(
            jax.ShapeDtypeStruct((8 * rows, width), LOW),
            jax.ShapeDtypeStruct((8 * rows, w.shape[1]), LOW),
            jax.ShapeDtypeStruct((8 * rows, w.shape[1]), LOW),
        ),
        in_specs=[INSIDE] * 5,
        out_specs=(ANYWHERE, INSIDE, INSIDE),
        scratch_shapes=gather_scratch(rows, width),
        compiler_params=pltpu.CompilerParams(collective_id=2, has_side_effects=True, vmem_limit_bytes=56 << 20),
        cost_estimate=LINK_COST,
    )(x, gain, shift, w, b)


def gather_mixed_kernel(x_ref, w_ref, whole, out_ref, held, send, recv, keep):
    rows = x_ref.shape[0]
    base = lax.axis_index("tensor") * rows
    held[stretch(base, rows), :] = x_ref[...]
    greet_tensor()

    def work(span):
        out_ref[span, :] = nt_dot(held[span, :], w_ref[...]).astype(LOW)

    gather_loop(rows, held, whole, send, recv, keep, work)


def gather_mixed(x, w):
    rows, width = x.shape
    return pl.pallas_call(
        gather_mixed_kernel,
        out_shape=(
            jax.ShapeDtypeStruct((8 * rows, width), LOW),
            jax.ShapeDtypeStruct((8 * rows, w.shape[0]), LOW),
        ),
        in_specs=[INSIDE] * 2,
        out_specs=(ANYWHERE, INSIDE),
        scratch_shapes=gather_scratch(rows, width),
        compiler_params=pltpu.CompilerParams(collective_id=3, has_side_effects=True, vmem_limit_bytes=48 << 20),
        cost_estimate=LINK_COST,
    )(x, w)


def scatter_steps(rows, make, o_ref, boxes, from_core, from_x, from_y, send, recv, unrolled=False):
    me, c, x, y, at = positions()
    tx, ty, tc = at(y, 1 - x, c), at(1 - y, x, c), at(y, x, 1 - c)
    half = rows // 2

    def remote(src, dst, index, peer):
        return pltpu.make_async_remote_copy(
            src_ref=src, dst_ref=dst, send_sem=send.at[index],
            recv_sem=recv.at[index], device_id={"tensor": peer}, device_id_type=MESH)

    def swap(k):
        return remote(boxes.at[k], from_core.at[k], k, tc)

    diagonal, beside_x, beside_y, own = (boxes.at[4 + k] for k in range(4))
    lo, hi = pl.ds(0, half), pl.ds(half, half)
    dx = remote(diagonal.at[lo, :], from_x.at[1, lo, :], 4, tx)
    dy = remote(diagonal.at[hi, :], from_y.at[1, hi, :], 5, ty)
    xl = remote(beside_x.at[lo, :], from_x.at[0, lo, :], 6, tx)
    xh = remote(beside_x.at[hi, :], from_x.at[0, hi, :], 7, tx)
    yl = remote(beside_y.at[lo, :], from_y.at[0, lo, :], 8, ty)
    yh = remote(beside_y.at[hi, :], from_y.at[0, hi, :], 9, ty)

    def produce(k):
        flip_x, flip_y = 1 - k // 2, 1 - k % 2
        chip = at(y + flip_y * (1 - 2 * y), x + flip_x * (1 - 2 * x), 0)

        @pl.loop(0, 2)
        def _(j):
            core = (1 - j) * (1 - c) + j * c
            make(stretch((chip + core) * rows, rows), boxes.at[4 * j + k])

            @pl.when(j == 0)
            def _():
                swap(k).start()

    def pass_diagonal():
        swap(0).wait_recv()
        add_into(diagonal, 0, half, diagonal, from_core.at[0])
        dx.start()
        add_into(diagonal, half, half, diagonal, from_core.at[0])
        dy.start()

    def pass_x():
        swap(1).wait_recv()
        add_into(beside_x, 0, half, beside_x, from_core.at[1])
        xl.start()

    def pass_y():
        swap(2).wait_recv()
        add_into(beside_y, half, half, beside_y, from_core.at[2])
        yh.start()

    if unrolled:
        produce(0)
        yield
        produce(1)
        pass_diagonal()
        yield
        produce(2)
        pass_x()
        yield
        produce(3)
        pass_y()
    else:
        @pl.loop(0, 4)
        def _(k):
            produce(k)
            pl.when(k == 1)(pass_diagonal)
            pl.when(k == 2)(pass_x)
            pl.when(k == 3)(pass_y)

    yield
    dy.wait_recv()
    add_into(beside_x, half, half, beside_x, from_core.at[1], from_y.at[1])
    xh.start()
    dx.wait_recv()
    add_into(beside_y, 0, half, beside_y, from_core.at[2], from_x.at[1])
    yl.start()
    yield
    swap(3).wait_recv()
    xl.wait_recv()
    yh.wait_recv()
    yield
    xh.wait_recv()
    yl.wait_recv()
    add_into(o_ref, 0, rows, own, from_core.at[3], from_x.at[0], from_y.at[0])
    for s in (swap(0), swap(1), swap(2), swap(3), dx, dy, xl, xh, yl, yh):
        s.wait_send()


def scatter_scratch(rows, width):
    return [
        pltpu.VMEM((8, rows, width), LOW),
        pltpu.VMEM((4, rows, width), LOW),
        pltpu.VMEM((2, rows, width), LOW),
        pltpu.VMEM((2, rows, width), LOW),
        pltpu.SemaphoreType.DMA((10,)),
        pltpu.SemaphoreType.DMA((10,)),
    ]


def tiles(count, size, body):
    @pl.loop(0, count // size)
    def _(tile):
        body(stretch(tile * size, size))


def project_scatter_kernel(a_ref, w_ref, o_ref, *scratch):
    rows = o_ref.shape[0]

    def make(span, box):
        def body(cols):
            box[:, cols] = nn_dot(a_ref[span, :], w_ref[:, cols]).astype(LOW)

        tiles(box.shape[1], 1024, body)

    greet_tensor()
    for _ in scatter_steps(rows, make, o_ref, *scratch):
        pass


def project_scatter(a, w):
    rows, width = a.shape[0] // 8, w.shape[1]
    return pl.pallas_call(
        project_scatter_kernel,
        out_shape=jax.ShapeDtypeStruct((rows, width), jnp.float32),
        in_specs=[INSIDE] * 2,
        out_specs=INSIDE,
        scratch_shapes=scatter_scratch(rows, width),
        compiler_params=pltpu.CompilerParams(collective_id=4, has_side_effects=True, vmem_limit_bytes=40 << 20),
        cost_estimate=LINK_COST,
    )(a, w)


def hidden_back_kernel(g_ref, slope_ref, down_ref, up_ref, o_ref, pre_ref, bias_ref, *scratch):
    rows = o_ref.shape[0]
    bias_ref[...] = jnp.zeros_like(bias_ref)

    def make(span, box):
        def first(cols):
            pre = (nt_dot(g_ref[span, :], down_ref[cols, :]) * slope_ref[span, cols].astype(jnp.float32)).astype(LOW)
            pre_ref[span, cols] = pre
            bias_ref[:, cols] += jnp.sum(pre.astype(jnp.float32), axis=0, keepdims=True)

        def second(cols):
            box[:, cols] = nt_dot(pre_ref[span, :], up_ref[cols, :]).astype(LOW)

        tiles(pre_ref.shape[1], 512, first)
        tiles(box.shape[1], 1024, second)

    greet_tensor()
    for _ in scatter_steps(rows, make, o_ref, *scratch):
        pass


def hidden_back(grad_rows, slope, down_weight, up_weight):
    rows, width = grad_rows.shape[0] // 8, grad_rows.shape[1]
    return pl.pallas_call(
        hidden_back_kernel,
        out_shape=(
            jax.ShapeDtypeStruct((rows, width), jnp.float32),
            jax.ShapeDtypeStruct(slope.shape, LOW),
            jax.ShapeDtypeStruct((1, slope.shape[1]), jnp.float32),
        ),
        in_specs=[INSIDE] * 4,
        out_specs=(INSIDE,) * 3,
        scratch_shapes=scatter_scratch(rows, width),
        compiler_params=pltpu.CompilerParams(collective_id=5, has_side_effects=True, vmem_limit_bytes=56 << 20),
        cost_estimate=LINK_COST,
    )(grad_rows, slope, down_weight, up_weight)


def line_steps(chunks, load, inward, across, outward):
    place = lax.axis_index("dp")
    outer = lax.rem(place, 3) == 0
    inner = lax.rem(place, 3) != 0
    near, beside, end = 1 + place // 3, 3 - place, (place - 1) * 3

    def remote(src, dst, sems, index, peer):
        return pltpu.make_async_remote_copy(
            src_ref=src, dst_ref=dst, send_sem=sems.at[0, index], recv_sem=sems.at[1, index],
            device_id={"dp": peer}, device_id_type=MESH)

    count = len(chunks)
    first = [remote(part, got, inward, k, near) for k, (part, own, got, out, prior) in enumerate(chunks)]
    second = [remote(own, out, across, k, beside) for k, (part, own, got, out, prior) in enumerate(chunks)]
    third = [remote(out, out, outward, k, end) for k, (part, own, got, out, prior) in enumerate(chunks)]
    loads = [
        pltpu.make_async_copy(part, own, load.at[k]) for k, (part, own, got, out, prior) in enumerate(chunks)
    ]
    ahead = 3

    @pl.when(outer)
    def _():
        for copy in first[:ahead]:
            copy.start()

    @pl.when(inner)
    def _():
        for copy in loads[:ahead]:
            copy.start()

    yield
    for step in range(count + 1):
        @pl.when(outer)
        def _(step=step):
            if step + ahead < count:
                first[step].wait_send()
                first[step + ahead].start()

        @pl.when(inner)
        def _(step=step):
            if step < count:
                part, own, got, out, prior = chunks[step]
                loads[step].wait()
                first[step].wait_recv()
                add_into(own, 0, own.shape[0], own, got)
                second[step].start()
            if step >= 1:
                part, own, got, out, prior = chunks[step - 1]
                second[step - 1].wait_recv()
                add_into(out, 0, out.shape[0], own, out)
                third[step - 1].start()
            if step + ahead < count:
                prior = chunks[step + ahead][4]
                if prior is not None:
                    second[prior].wait_send()
                loads[step + ahead].start()
        yield

    @pl.when(outer)
    def _():
        for k in range(max(0, count - ahead), count):
            first[k].wait_send()
        for copy in third:
            copy.wait_recv()

    @pl.when(inner)
    def _():
        reused = [chunk[4] for chunk in chunks]
        for k in range(count):
            if k not in reused:
                second[k].wait_send()
            third[k].wait_send()


SLOTS = 6


def chunk_shape(part):
    if len(part.shape) == 3:
        return (HALF_MEGA // part.shape[2], part.shape[2])
    return (HALF_MEGA // part.shape[1], part.shape[1])


def line_chunks(parts, own, got, outs):
    chunks = []
    for part, box, landing, out in zip(parts, own, got, outs):
        size = chunk_shape(part)[0]
        if len(part.shape) == 3:
            views = [
                (lead, pl.ds(first, size), slice(None))
                for lead in range(part.shape[0])
                for first in range(0, part.shape[1], size)
            ]
        else:
            views = [(pl.ds(first, size), slice(None)) for first in range(0, part.shape[0], size)]
        base = len(chunks)
        for k, view in enumerate(views):
            prior = base + k - SLOTS if k >= SLOTS else None
            chunks.append((part.at[view], box.at[k % SLOTS], landing.at[view], out.at[view], prior))
    return chunks


def shared_steps(v_ref, total, got, far, send, recv, everyone):
    me, c, x, y, at = positions()
    place = lax.axis_index("dp")
    count = lax.axis_size("dp")
    for k, peer in enumerate((at(y, x, 1 - c), at(y, 1 - x, c), at(1 - y, x, c))):
        swap = pltpu.make_async_remote_copy(
            src_ref=total.at[k], dst_ref=got.at[k], send_sem=send.at[k], recv_sem=recv.at[k],
            device_id={"tensor": peer}, device_id_type=MESH)
        swap.start()
        yield
        swap.wait()
        total[k + 1, :everyone, :] = total[k, :everyone, :] + got[k, :everyone, :]
        total[k + 1, everyone:, :] = total[k, everyone:, :]
    far[place] = total[3]
    swaps = [
        pltpu.make_async_remote_copy(
            src_ref=total.at[3], dst_ref=far.at[place], send_sem=send.at[2 + k], recv_sem=recv.at[2 + k],
            device_id={"dp": lax.rem(place + k, count)}, device_id_type=MESH)
        for k in range(1, count)
    ]
    for swap in swaps:
        swap.start()
    yield
    yield
    for swap in swaps:
        swap.wait()
    acc = far[0]
    for k in range(1, count):
        acc = acc + far[k]
    v_ref[...] = acc


def closing_kernel(amount, *refs):
    joined_ref, w_ref, x_ref, gain_ref, middle_ref, known_ref, hidden_ref, down_ref = refs[:8]
    parts, refs = refs[8 : 8 + amount], refs[8 + amount :]
    late_out, input_out, shared_out = refs[:3]
    outs, rest = refs[3 : 3 + amount], refs[3 + amount :]
    own, got, rest = rest[:amount], rest[amount : 2 * amount], rest[2 * amount :]
    load, inward, across, outward, grad_ref, total, near, far, near_send, near_recv, credit, local = rest[:12]
    hidden_box, down_box, down_sem = rest[12:15]
    boxes, from_core, from_x, from_y, send, recv, late_send, late_recv = rest[15:]
    rows = x_ref.shape[0]
    me, c, x, y, at = positions()
    place = lax.axis_index("dp")
    count = lax.axis_size("dp")
    around = (at(y, 1 - x, c), at(1 - y, x, c), at(y, x, 1 - c))

    barrier = pltpu.get_barrier_semaphore()
    for peer in around:
        pl.semaphore_signal(barrier, inc=1, device_id={"tensor": peer}, device_id_type=MESH)
    for k in range(1, count):
        pl.semaphore_signal(barrier, inc=1, device_id={"dp": lax.rem(place + k, count)}, device_id_type=MESH)
    pl.semaphore_wait(barrier, 3 + count - 1)

    def make(span, box):
        def body(cols):
            acc = nt_dot(joined_ref[0, span, :], w_ref[0, cols, :])
            for part in (1, 2):
                acc = acc + nt_dot(joined_ref[part, span, :], w_ref[part, cols, :])
            box[:, cols] = acc.astype(LOW)

        tiles(box.shape[1], 1024, body)

    def make_late(span, box):
        copy = pltpu.make_async_copy(hidden_ref.at[span, :], hidden_box, local)
        copy.start()
        copy.wait()

        def body(cols):
            box[:, cols] = nn_dot(hidden_box[...], down_box[:, cols]).astype(LOW)

        tiles(box.shape[1], 1024, body)

    fill = pltpu.make_async_copy(down_ref, down_box, down_sem)
    fill.start()
    line = line_steps(line_chunks(parts, own, got, outs), load, inward, across, outward)
    next(line)
    for _ in scatter_steps(rows, make, grad_ref, boxes, from_core, from_x, from_y, send, recv, True):
        next(line)
        next(line)
    for peer in around:
        pl.semaphore_signal(credit, inc=1, device_id={"tensor": peer}, device_id_type=MESH)

    total[0] = known_ref[...]

    @pl.loop(0, rows // TILE)
    def _(step):
        span = stretch(step * TILE, TILE)
        unit, inverse = standardize(x_ref[span, :].astype(jnp.float32))
        grad = grad_ref[span, :]
        scaled = grad * gain_ref[...]
        inner = jnp.mean(scaled * unit, axis=-1, keepdims=True)
        part = (scaled - jnp.mean(scaled, axis=-1, keepdims=True) - unit * inner) * inverse
        input_out[span, :] = middle_ref[span, :] + part
        total[0, 0:1, :] += jnp.sum(grad * unit, axis=0, keepdims=True)
        total[0, 1:2, :] += jnp.sum(grad, axis=0, keepdims=True)

    next(line)
    pl.semaphore_wait(credit, 3)
    fill.wait()
    for _ in scatter_steps(rows, make_late, late_out, boxes, from_core, from_x, from_y, late_send, late_recv, True):
        next(line)
        next(line)
    for _ in shared_steps(shared_out, total, near, far, near_send, near_recv, 6):
        next(line)
    for _ in line:
        pass


def closing_sums(joined_grad, qkv, inputs, gain, middle_grad, known, hidden, down_weight, parts):
    rows, width = inputs.shape
    amount = len(parts)
    chunks = sum(part.size for part in parts) // HALF_MEGA
    count = lax.axis_size("dp")
    pairs = pltpu.SemaphoreType.DMA((2, chunks))
    scatter = scatter_scratch(rows, width)
    return pl.pallas_call(
        functools.partial(closing_kernel, amount),
        out_shape=(
            jax.ShapeDtypeStruct((rows, width), jnp.float32),
            jax.ShapeDtypeStruct((rows, width), jnp.float32),
            jax.ShapeDtypeStruct(known.shape, jnp.float32),
        )
        + tuple(jax.ShapeDtypeStruct(part.shape, LOW) for part in parts),
        in_specs=[INSIDE] * 6 + [ANYWHERE] * (2 + amount),
        out_specs=(INSIDE,) * (3 + amount),
        scratch_shapes=[pltpu.VMEM((SLOTS,) + chunk_shape(part), LOW) for part in parts]
        + [pltpu.VMEM(part.shape, LOW) for part in parts]
        + [
            pltpu.SemaphoreType.DMA((chunks,)), pairs, pairs, pairs,
            pltpu.VMEM((rows, width), jnp.float32),
            pltpu.VMEM((4,) + known.shape, jnp.float32),
            pltpu.VMEM((3,) + known.shape, jnp.float32),
            pltpu.VMEM((count,) + known.shape, jnp.float32),
            pltpu.SemaphoreType.DMA((3 + count - 1,)),
            pltpu.SemaphoreType.DMA((3 + count - 1,)),
            pltpu.SemaphoreType.REGULAR,
            pltpu.SemaphoreType.DMA,
            pltpu.VMEM((rows, hidden.shape[1]), LOW),
            pltpu.VMEM(down_weight.shape, LOW),
            pltpu.SemaphoreType.DMA,
        ]
        + scatter + scatter[4:],
        compiler_params=pltpu.CompilerParams(collective_id=6, has_side_effects=True, vmem_limit_bytes=60 << 20),
        cost_estimate=LINK_COST,
    )(joined_grad, qkv, inputs, gain, middle_grad, known, hidden, down_weight, *parts)


def first_positions(lengths_ref, row, base, count):
    places = base + lax.broadcasted_iota(jnp.int32, (1, count), 1)
    begin = jnp.int32(0)
    first = jnp.zeros((1, count), jnp.int32)
    for doc in range(lengths_ref.shape[1] - 1):
        begin = begin + lengths_ref[row, doc]
        first = jnp.where(places >= begin, begin, first)
    return places, first


def masked_scores(lengths_ref, query_rows, key_rows, first_key, first_query):
    keys, queries = key_rows.shape[0], query_rows.shape[0]
    scores = nt_dot(key_rows, query_rows) * HD ** (-0.5)
    places, first = first_positions(lengths_ref, pl.program_id(0), first_query, queries)
    key_places = first_key + lax.broadcasted_iota(jnp.int32, (keys, queries), 0)
    allowed = (key_places >= first) & (key_places <= places)
    return scores, allowed


def attend_kernel(lengths_ref, joined_ref, out_ref, log_ref):
    length, width = out_ref.shape
    for head in range(width // HD):
        cols = slice(head * HD, (head + 1) * HD)
        value_t = joined_ref[2, :, cols].T
        for block in range(length // QUERY_BLOCK):
            first, stop = block * QUERY_BLOCK, (block + 1) * QUERY_BLOCK
            start = max(0, first - MOST_DOC)
            scores, allowed = masked_scores(
                lengths_ref, joined_ref[0, first:stop, cols], joined_ref[1, start:stop, cols], start, first)
            scores = jnp.where(allowed, scores, -1000000000.0)
            row_max = jnp.max(scores, axis=0, keepdims=True)
            exp_scores = jnp.exp(scores - row_max)
            row_total = jnp.sum(exp_scores, axis=0, keepdims=True)
            prob_low = (exp_scores * (1.0 / row_total)).astype(LOW)
            out_ref[first:stop, cols] = nn_dot(value_t[:, start:stop], prob_low).T.astype(LOW)
            log_ref[head : head + 1, first:stop] = row_max + jnp.log(row_total)


def attend(lengths, joined):
    rows = lengths.shape[0]
    tokens, width = joined.shape[1], joined.shape[2]
    length, heads = tokens // rows, width // HD
    area = rows * heads * length * MOST_DOC
    return pl.pallas_call(
        attend_kernel,
        grid=(rows,),
        out_shape=(
            jax.ShapeDtypeStruct((tokens, width), LOW),
            jax.ShapeDtypeStruct((rows, heads, length), jnp.float32),
        ),
        in_specs=[
            pl.BlockSpec(memory_space=pltpu.SMEM),
            pl.BlockSpec((3, length, width), lambda row: (0, row, 0)),
        ],
        out_specs=(
            pl.BlockSpec((length, width), lambda row: (row, 0)),
            pl.BlockSpec((None, heads, length), lambda row: (row, 0, 0)),
        ),
        compiler_params=pltpu.CompilerParams(vmem_limit_bytes=40 << 20),
        cost_estimate=pl.CostEstimate(flops=4 * area * HD, bytes_accessed=8 * tokens * width, transcendentals=area),
    )(lengths, joined)


def attend_back_kernel(lengths_ref, joined_ref, mixed_ref, log_ref, out_ref, sum_ref, key_acc, value_acc):
    length, width = mixed_ref.shape
    scale = HD ** (-0.5)
    for head in range(width // HD):
        cols = slice(head * HD, (head + 1) * HD)
        key_t = joined_ref[1, :, cols].T
        key_acc[...] = jnp.zeros_like(key_acc)
        value_acc[...] = jnp.zeros_like(value_acc)
        query_total = jnp.zeros((1, HD), jnp.float32)
        for block in range(length // QUERY_BLOCK):
            first, stop = block * QUERY_BLOCK, (block + 1) * QUERY_BLOCK
            start = max(0, first - MOST_DOC)
            query_rows = joined_ref[0, first:stop, cols]
            mixed_rows = mixed_ref[first:stop, cols]
            scores, allowed = masked_scores(
                lengths_ref, query_rows, joined_ref[1, start:stop, cols], start, first)
            prob = jnp.where(allowed, jnp.exp(scores - log_ref[head : head + 1, first:stop]), 0.0)
            prob_grad = nt_dot(joined_ref[2, start:stop, cols], mixed_rows)
            inner = jnp.sum(prob * prob_grad, axis=0, keepdims=True)
            score_grad = (prob * (prob_grad - inner)).astype(LOW)
            query_grad = (nn_dot(key_t[:, start:stop], score_grad) * scale).T.astype(LOW)
            out_ref[0, first:stop, cols] = query_grad
            query_total = query_total + jnp.sum(query_grad.astype(jnp.float32), axis=0, keepdims=True)
            key_acc[start:stop, :] += nn_dot(score_grad, query_rows)
            value_acc[start:stop, :] += nn_dot(prob.astype(LOW), mixed_rows)
        value_grad = value_acc[...].astype(LOW)
        out_ref[1, :, cols] = (key_acc[...] * scale).astype(LOW)
        out_ref[2, :, cols] = value_grad
        sum_ref[0:1, cols] = query_total
        sum_ref[1:2, cols] = jnp.sum(value_grad.astype(jnp.float32), axis=0, keepdims=True)


def attend_back(lengths, joined, mixed_grad, log_total):
    rows = lengths.shape[0]
    tokens, width = mixed_grad.shape
    length, heads = tokens // rows, width // HD
    area = rows * heads * length * MOST_DOC
    return pl.pallas_call(
        attend_back_kernel,
        grid=(rows,),
        out_shape=(
            jax.ShapeDtypeStruct((3, tokens, width), LOW),
            jax.ShapeDtypeStruct((rows, 2, width), jnp.float32),
        ),
        in_specs=[
            pl.BlockSpec(memory_space=pltpu.SMEM),
            pl.BlockSpec((3, length, width), lambda row: (0, row, 0)),
            pl.BlockSpec((length, width), lambda row: (row, 0)),
            pl.BlockSpec((None, heads, length), lambda row: (row, 0, 0)),
        ],
        out_specs=(
            pl.BlockSpec((3, length, width), lambda row: (0, row, 0)),
            pl.BlockSpec((None, 2, width), lambda row: (row, 0, 0)),
        ),
        scratch_shapes=[pltpu.VMEM((length, HD), jnp.float32), pltpu.VMEM((length, HD), jnp.float32)],
        compiler_params=pltpu.CompilerParams(vmem_limit_bytes=40 << 20),
        cost_estimate=pl.CostEstimate(flops=10 * area * HD, bytes_accessed=16 * tokens * width, transcendentals=area),
    )(lengths, joined, mixed_grad, log_total)


def norm_back(unit, inverse, grad, gain):
    scaled = grad * gain
    inner = jnp.mean(scaled * unit, axis=-1, keepdims=True)
    part = (scaled - jnp.mean(scaled, axis=-1, keepdims=True) - unit * inner) * inverse
    return part, jnp.sum(grad * unit, axis=0), jnp.sum(grad, axis=0)


def after(value, *anchors):
    return lax.optimization_barrier((value,) + anchors)[0]


def shards(
    inputs,
    doc_lengths,
    attn_gain,
    attn_shift,
    qkv_weight,
    qv_bias,
    out_weight,
    out_bias,
    mlp_gain,
    mlp_shift,
    up_weight,
    up_bias,
    down_weight,
    down_bias,
    out_grad,
):
    fast = lax.axis_size("tensor") == 8 and lax.axis_size("dp") == 4

    def wide(vector):
        return vector.astype(jnp.float32)[None, :]

    def gather(block):
        return lax.all_gather(block, "tensor", axis=0, tiled=True)

    def scatter(partial):
        return lax.psum_scatter(partial, "tensor", scatter_dimension=0, tiled=True)

    qkv = qkv_weight.transpose(1, 0, 2)
    bias = jnp.stack([qv_bias[0], jnp.zeros_like(qv_bias[0]), qv_bias[1]]).astype(jnp.float32)[:, None, :]
    inputs32 = inputs.astype(jnp.float32)
    if fast:
        attn_rows, joined = gather_project(inputs, wide(attn_gain), wide(attn_shift), qkv, bias)
    else:
        attn_unit, attn_inverse = standardize(inputs32)
        attn_rows = gather((attn_unit * wide(attn_gain) + wide(attn_shift)).astype(LOW))
        joined = jnp.einsum("td,cdh->cth", attn_rows, qkv, preferred_element_type=jnp.float32)
        joined = (joined + bias).astype(LOW)
    grad_rows = gather(after(out_grad, attn_rows))
    heads_out, log_total = attend(doc_lengths, joined)
    if fast:
        attn_sum = project_scatter(heads_out, out_weight)
    else:
        attn_sum = scatter(nn_dot(heads_out, out_weight))
    middle = inputs32 + attn_sum + out_bias
    mlp_unit, mlp_inverse = standardize(middle)
    if fast:
        mlp_rows, hidden, slope = gather_hidden(middle, wide(mlp_gain), wide(mlp_shift), up_weight, wide(up_bias))
    else:
        mlp_rows = gather((mlp_unit * wide(mlp_gain) + wide(mlp_shift)).astype(LOW))
        hidden, slope = gelu_pair(nn_dot(mlp_rows, up_weight) + up_bias)
        hidden = hidden.astype(LOW)
    down_part = contract_first(hidden, grad_rows)
    if fast:
        down_part = down_part.astype(LOW)
        down_sum = lax.psum(down_part, "dp").astype(jnp.float32)
        mlp_norm_grad, pre_grad, up_bias_grad = hidden_back(after(grad_rows, down_part), slope, down_weight, up_weight)
        up_bias_grad = up_bias_grad[0]
    else:
        pre_grad = (nt_dot(grad_rows, down_weight) * slope).astype(LOW)
        up_bias_grad = jnp.sum(pre_grad, axis=0, dtype=jnp.float32)
        mlp_norm_grad = scatter(nt_dot(pre_grad, up_weight))
    up_part = contract_first(mlp_rows, pre_grad)
    grad32 = out_grad.astype(jnp.float32)
    down_bias_grad = jnp.sum(grad32, axis=0)
    middle_part, mlp_gain_grad, mlp_shift_grad = norm_back(mlp_unit, mlp_inverse, mlp_norm_grad, wide(mlp_gain))
    middle_grad = grad32 + middle_part
    out_bias_grad = jnp.sum(middle_grad, axis=0)
    if fast:
        middle_rows, mixed_grad = gather_mixed(middle_grad.astype(LOW), out_weight)
    else:
        middle_rows = gather(middle_grad.astype(LOW))
        mixed_grad = nt_dot(middle_rows, out_weight).astype(LOW)
    out_part = contract_first(heads_out, middle_rows)
    joined_grad, bias_sums = attend_back(doc_lengths, joined, mixed_grad, log_total)
    qkv_part = jnp.einsum("td,cth->cdh", attn_rows, joined_grad, preferred_element_type=jnp.float32)
    qv_bias_grad = jnp.sum(bias_sums, axis=0)
    shared = [out_bias_grad, mlp_gain_grad, mlp_shift_grad, down_bias_grad]
    if fast:
        own = jnp.concatenate([up_bias_grad, qv_bias_grad.reshape(-1)])
        own = jnp.pad(own, (0, 2 * inputs.shape[1] - own.shape[0])).reshape(2, -1)
        known = jnp.concatenate([jnp.zeros((2, inputs.shape[1]), jnp.float32), jnp.stack(shared), own])
        mlp_sum, input_grad, summed, up_sum, out_sum, qkv_sum = closing_sums(
            joined_grad, qkv, inputs, wide(attn_gain), middle_grad, known, hidden, down_weight,
            [up_part.astype(LOW), out_part.astype(LOW), qkv_part.astype(LOW)])
        up_sum, out_sum, qkv_sum = (part.astype(jnp.float32) for part in (up_sum, out_sum, qkv_sum))
        shared = [summed[index] for index in range(6)]
        own = summed[6:].reshape(-1)
        up_bias_grad = own[: up_bias_grad.shape[0]]
        qv_bias_grad = own[up_bias_grad.shape[0] :][: qv_bias_grad.size].reshape(qv_bias_grad.shape)
    else:
        attn_part = jnp.einsum("cth,cdh->td", joined_grad, qkv, preferred_element_type=jnp.float32)
        input_part, attn_gain_grad, attn_shift_grad = norm_back(
            attn_unit, attn_inverse, scatter(attn_part), wide(attn_gain))
        input_grad = middle_grad + input_part
        mlp_sum = scatter(nn_dot(hidden, down_weight))
        shared = lax.psum([attn_gain_grad, attn_shift_grad] + shared, ("dp", "tensor"))
        up_bias_grad, qv_bias_grad = lax.psum((up_bias_grad, qv_bias_grad), "dp")
        down_sum, up_sum, out_sum, qkv_sum = lax.psum((down_part, up_part, out_part, qkv_part), "dp")
    outputs = (middle + mlp_sum + down_bias).astype(LOW)
    return (
        outputs,
        input_grad,
        shared[0],
        shared[1],
        qkv_sum.transpose(1, 0, 2),
        qv_bias_grad,
        out_sum,
        shared[2],
        shared[3],
        shared[4],
        up_sum,
        up_bias_grad,
        down_sum,
        shared[5],
    )


def solution(mesh):
    return jax.shard_map(
        shards,
        mesh=mesh,
        in_specs=(
            P(("dp", "tensor"), None),
            P("dp", None),
            P(),
            P(),
            P(None, None, "tensor"),
            P(None, "tensor"),
            P("tensor", None),
            P(),
            P(),
            P(),
            P(None, "tensor"),
            P("tensor"),
            P("tensor", None),
            P(),
            P(("dp", "tensor"), None),
        ),
        out_specs=(
            P(("dp", "tensor"), None),
            P(("dp", "tensor"), None),
            P(),
            P(),
            P(None, None, "tensor"),
            P(None, "tensor"),
            P("tensor", None),
            P(),
            P(),
            P(),
            P(None, "tensor"),
            P("tensor"),
            P("tensor", None),
            P(),
        ),
        check_vma=False,
    )
```
